8 devices in a mesh: batch: 1 (over z), row: 2 (over y), col: 4 (over x, core).
Axes of the slice: x: 2, y: 2, z: 1, core: 2. Of those that a mesh axis runs over, the one named last changes fastest.
Arguments:
- spd_blocks: float32 [16, 384, 6144], P(('batch', 'row'), None, 'col')
Outputs:
- output: float32 [16, 384, 6144], P(('batch', 'row'), None, 'col')
All inputs are finite; a program needn't handle non-finite values.
Results may differ from the reference program's by a relative error of at most 0.001.
Values are sent between devices in bfloat16 or wider.
A program may use at most 1 GiB of HBM per device.

```python
import math
import jax
import jax.numpy as jnp
from jax import lax

BLOCK = 384
ORDER = 6144
ROW_DEVS = 2
COL_DEVS = 4

BLOCK_COUNT = ORDER // BLOCK


def to_logical(a_cyc):
    by_rows = a_cyc.reshape(ROW_DEVS, BLOCK_COUNT // ROW_DEVS, BLOCK, ORDER).transpose(1, 0, 2, 3)
    by_cols = by_rows.reshape(ORDER, COL_DEVS, BLOCK_COUNT // COL_DEVS, BLOCK).transpose(0, 2, 1, 3)
    return by_cols.reshape(ORDER, ORDER)


def to_cyclic(matrix):
    by_rows = matrix.reshape(BLOCK_COUNT // ROW_DEVS, ROW_DEVS, BLOCK, ORDER).transpose(1, 0, 2, 3)
    by_cols = by_rows.reshape(ORDER, BLOCK_COUNT // COL_DEVS, COL_DEVS, BLOCK).transpose(0, 2, 1, 3)
    return by_cols.reshape(BLOCK_COUNT, BLOCK, ORDER)


def setup_inputs(seed: int = 0, part: int = 0) -> dict:
    rng_key = jax.random.fold_in(jax.random.key(seed), part)
    gauss_draw = jax.random.normal(rng_key, (ORDER, ORDER), jnp.float32)
    sym_part = (gauss_draw + gauss_draw.T) * math.sqrt(0.5 / ORDER)
    matrix = (sym_part + 2.2 * jnp.eye(ORDER, dtype=jnp.float32)) * ORDER
    return {"spd_blocks": to_cyclic(matrix)}


def reference(spd_blocks):
    trailing = to_logical(spd_blocks)
    columns = []
    for step_idx in range(BLOCK_COUNT):
        diag_fac = jnp.tril(jnp.linalg.cholesky(trailing[:BLOCK, :BLOCK]))
        pieces = [jnp.zeros((step_idx * BLOCK, BLOCK), jnp.float32), diag_fac]
        if step_idx + 1 < BLOCK_COUNT:
            panel_f32 = lax.linalg.triangular_solve(diag_fac, trailing[BLOCK:, :BLOCK], left_side=False, lower=True, transpose_a=True)
            pieces.append(panel_f32)
            panel_b16 = panel_f32.astype(jnp.bfloat16)
            trailing = trailing[BLOCK:, BLOCK:] - jnp.dot(panel_b16, panel_b16.T, preferred_element_type=jnp.float32)
        columns.append(jnp.concatenate(pieces, axis=0))
    return to_cyclic(jnp.concatenate(columns, axis=1))
```

```python
import functools
import jax
import jax.numpy as jnp
from jax import lax
from jax.experimental import pallas as pl
from jax.experimental.pallas import tpu as pltpu
from jax.sharding import PartitionSpec as P

F32 = jnp.float32
BF16 = jnp.bfloat16
NB = 16
BS = 384
SUB = 128
MESH = pl.DeviceIdType.MESH


def dot_hi(a, b, dims):
    return lax.dot_general(a, b, (dims, ((), ())), precision=lax.Precision.HIGHEST, preferred_element_type=F32)


def lane_splat(x, i):
    return jnp.broadcast_to(x[:, i:i + 1], (8, SUB))


def row_splat(ref, row):
    return jnp.broadcast_to(ref[row:row + 1, :], (8, SUB))


def factor_tile(d_ref, off, u_ref, w_ref, sc):
    lane = lax.broadcasted_iota(jnp.int32, (8, SUB), 1)
    sub = lax.broadcasted_iota(jnp.int32, (8, SUB), 0)
    n_oct = SUB // 8
    X = [d_ref[pl.ds(pl.multiple_of(off + 8 * t, 8), 8), pl.ds(off, SUB)] for t in range(n_oct)]
    nxt = [lane_splat(X[0], i) for i in range(8)]
    for t in range(n_oct):
        j = 8 * t
        o = 160 * (t % 2)
        rows = X[t]
        for i in range(8):
            sc[o + 8 * i:o + 8 * i + 8, :] = nxt[i]
        d = {(m, i): row_splat(sc, o + 8 * i + m) for i in range(8) for m in range(i, 8)}
        sc[o + 64:o + 72, :] = rows
        sc[o + 72:o + 80, :] = jnp.where(lane < j, rows, jnp.where(lane == sub + j, 1.0, 0.0))
        inv = [None] * 8
        low = {}
        for i in range(8):
            inv[i] = lax.rsqrt(d[i, i])
            for m in range(i + 1, 8):
                low[m, i] = d[m, i] * inv[i]
            for m in range(i + 1, 8):
                for n in range(i + 1, m + 1):
                    d[m, n] = d[m, n] - low[m, i] * low[n, i]

        def column(s):
            c = []
            for i in range(8):
                x = lane_splat(X[s], j + i)
                for p in range(i):
                    x = x - low[i, p] * c[p]
                c.append(x * inv[i])
            return c

        if t + 1 < n_oct:
            first = column(t + 1)
            nxt = [lane_splat(X[t + 1], j + 8 + m) for m in range(8)]
            for i in range(8):
                sc[o + 80 + 8 * i:o + 88 + 8 * i, :] = first[i]
            for i in range(8):
                for m in range(8):
                    nxt[m] = nxt[m] - first[i] * row_splat(sc, o + 80 + 8 * i + m)
        u = []
        w = []
        for i in range(8):
            x = row_splat(sc, o + 64 + i)
            y = row_splat(sc, o + 72 + i)
            for p in range(i):
                x = x - low[i, p] * u[p]
                y = y - low[i, p] * w[p]
            u.append(x * inv[i])
            w.append(y * inv[i])
        u8 = u[7]
        w8 = w[7]
        for i in range(7):
            u8 = jnp.where(sub == i, u[i], u8)
            w8 = jnp.where(sub == i, w[i], w8)
        u_ref[j:j + 8, :] = jnp.where(lane >= sub + j, u8, 0.0)
        w_ref[j:j + 8, :] = jnp.where(lane < j + 8, w8, 0.0)
        z = [jnp.where(lane < j + 8, w[i], u[i]) for i in range(8)]
        for s in range(t + 1, n_oct):
            c = first if s == t + 1 else column(s)
            x = jnp.where((lane >= j) & (lane < j + 8), 0.0, X[s])
            for i in range(8):
                x = x - c[i] * z[i]
            X[s] = x


def kernel(a_hbm, o_hbm, S, PQ, FB, D, ub, wb, sc, ld_sem, st_sem, send_sem, p_sem, q_sem, fs_sem, fr_sem):
    g = lax.axis_index("batch")
    r = lax.axis_index("row")
    c = lax.axis_index("col")
    n_q0 = 64
    same = r == lax.rem(c, 2)

    def blk(s):
        return pl.ds(pl.multiple_of(s * BS, SUB), BS)

    def p_idx(k, t):
        return 8 * k - (k // 2) * ((k + 1) // 2) + t - (k + 1) // 2

    def q_idx(k, s):
        m = k // 4
        return 4 * k - (4 * (m * (m - 1) // 2) + (k - 4 * m) * m) + s - m

    def first_t(k):
        return (k + 2 - r) // 2

    def first_s(k):
        return (k + 4 - c) // 4

    def relay(k):
        return 2 - 2 * (lax.rem(k, 4) // 2)

    def to(row, col):
        return (g, row, col)

    def p_copy(k, t, kind, col):
        i = p_idx(k, t)
        return pltpu.make_async_remote_copy(PQ.at[i], PQ.at[i], send_sem.at[kind, i], p_sem.at[i],
                                            device_id=to(r, col), device_id_type=MESH)

    def q_copy(k, t):
        i = p_idx(k, t)
        q = q_idx(k, (2 * t + r - c) // 4)
        return pltpu.make_async_remote_copy(PQ.at[i], PQ.at[n_q0 + q], send_sem.at[2, i], q_sem.at[q],
                                            device_id=to(1 - r, c), device_id_type=MESH)

    def p_local(k, t):
        i = p_idx(k, t)
        return pltpu.make_async_remote_copy(PQ.at[i], PQ.at[i], send_sem.at[0, i], p_sem.at[i],
                                            device_id=to(r, c ^ 1), device_id_type=MESH)

    def q_local(k, s):
        q = q_idx(k, s)
        return pltpu.make_async_remote_copy(PQ.at[n_q0 + q], PQ.at[n_q0 + q], send_sem.at[2, 0], q_sem.at[q],
                                            device_id=to(1 - r, c), device_id_type=MESH)

    def each_send(k, t, act):
        kc = lax.rem(k, 4)
        i = 2 * t + r
        odd = lax.rem(k, 2)
        far = i > k + 1
        own = c == kc

        @pl.when(own & (far | (odd == 0)))
        def _():
            act(p_copy(k, t, 0, c ^ 1))

        @pl.when(own & (far | (odd == 1)))
        def _():
            act(p_copy(k, t, 1, relay(k)))

        @pl.when((c == relay(k)) & far)
        def _():
            act(p_copy(k, t, 0, c ^ 1))

        @pl.when(same & (lax.rem(i, 4) == c) & (own | far | (c == lax.rem(k + 1, 4))))
        def _():
            act(q_copy(k, t))

    def recv(k, t):
        p_local(k, t).wait_recv()
        each_send(k, t, lambda cp: cp.start())

    def col_index(k, s):
        return jnp.where(same, p_idx(k, 2 * s + (c - r) // 2), n_q0 + q_idx(k, s))

    def update(k, t, s):
        prod = lax.dot_general(PQ[p_idx(k, t)], PQ[col_index(k, s)], (((1,), (1,)), ((), ())),
                               preferred_element_type=F32)
        S[t, :, blk(s)] = S[t, :, blk(s)] - prod

    def fb_copy(slot, b):
        view = FB.at[slot, b, :, SUB * b:BS]
        return pltpu.make_async_remote_copy(view, view, fs_sem.at[slot, b], fr_sem.at[slot, b],
                                            device_id=to(1 - r, c), device_id_type=MESH)

    def load(t, s):
        return pltpu.make_async_copy(a_hbm.at[t, :, blk(s)], S.at[t, :, blk(s)], ld_sem.at[t, s])

    def store(t, s):
        return pltpu.make_async_copy(S.at[t, :, blk(s)], o_hbm.at[t, :, blk(s)], st_sem.at[t, s])

    def lower(t, s):
        return 2 * t + r >= 4 * s + c

    barrier = pltpu.get_barrier_semaphore()

    def all_blocks(fn):
        def body(n, _):
            fn(n // 4, lax.rem(n, 4))
            return 0
        lax.fori_loop(0, 32, body, 0)

    def begin(t, s):
        @pl.when(lower(t, s))
        def _():
            load(t, s).start()

    def blank(t, s):
        @pl.when(jnp.logical_not(lower(t, s)))
        def _():
            S[t, :, blk(s)] = jnp.zeros((BS, BS), F32)
            store(t, s).start()

    def arrived(t, s):
        @pl.when(lower(t, s))
        def _():
            load(t, s).wait()

    all_blocks(begin)
    for step in range(1, 8):
        dr, dc = step // 4, step % 4
        pl.semaphore_signal(barrier, inc=1, device_id=to(r ^ dr, c ^ dc), device_id_type=MESH)
    all_blocks(blank)
    pl.semaphore_wait(barrier, 7)
    all_blocks(arrived)

    def factor_diag(slot):
        def tile(b, _):
            off = pl.multiple_of(b * SUB, SUB)
            factor_tile(D, off, ub.at[b], wb, sc)
            w = wb[...]
            FB[slot, b, :, pl.ds(off, SUB)] = w

            @pl.when(b == 0)
            def _():
                rest = dot_hi(w, D[0:SUB, SUB:BS], ((1,), (0,)))
                FB[slot, 0, :, SUB:BS] = rest
                fb_copy(slot, 0).start()
                D[SUB:BS, SUB:BS] = D[SUB:BS, SUB:BS] - dot_hi(rest, rest, ((0,), (0,)))

            @pl.when(b == 1)
            def _():
                rest = dot_hi(w, D[SUB:2 * SUB, 2 * SUB:BS], ((1,), (0,)))
                FB[slot, 1, :, 2 * SUB:BS] = rest
                fb_copy(slot, 1).start()
                D[2 * SUB:BS, 2 * SUB:BS] = D[2 * SUB:BS, 2 * SUB:BS] - dot_hi(rest, rest, ((0,), (0,)))

            @pl.when(b == 2)
            def _():
                fb_copy(slot, 2).start()
            return 0
        lax.fori_loop(0, 3, tile, 0)

    def solve(k, t, s):
        x1 = dot_hi(S[t, :, pl.ds(pl.multiple_of(s * BS, SUB), SUB)], FB[s, 0, :, 0:SUB], ((1,), (1,)))
        s2 = S[t, :, pl.ds(pl.multiple_of(s * BS + SUB, SUB), SUB)] - dot_hi(x1, FB[s, 0, :, SUB:2 * SUB], ((1,), (0,)))
        x2 = dot_hi(s2, FB[s, 1, :, SUB:2 * SUB], ((1,), (1,)))
        s3 = S[t, :, pl.ds(pl.multiple_of(s * BS + 2 * SUB, SUB), SUB)] - dot_hi(x1, FB[s, 0, :, 2 * SUB:BS], ((1,), (0,)))
        s3 = s3 - dot_hi(x2, FB[s, 1, :, 2 * SUB:BS], ((1,), (0,)))
        x3 = dot_hi(s3, FB[s, 2, :, 2 * SUB:BS], ((1,), (1,)))
        i = p_idx(k, t)
        for n, x in enumerate((x1, x2, x3)):
            PQ[i, :, SUB * n:SUB * (n + 1)] = x.astype(BF16)
            S[t, :, pl.ds(pl.multiple_of(s * BS + SUB * n, SUB), SUB)] = x

    def body(k, _):
        kc = lax.rem(k, 4)
        kr = lax.rem(k, 2)
        sk = k // 4
        tk = k // 2
        own = c == kc
        t0 = first_t(k)

        @pl.when(own)
        def _():
            @pl.when(r == kr)
            def _():
                @pl.when(k > 0)
                def _():
                    recv(k - 1, tk)
                    update(k - 1, tk, sk)
                D[...] = S[tk, :, blk(sk)]
                factor_diag(sk)

            @pl.when((r != kr) & (k > 0))
            def _():
                q_local(k - 1, sk).wait_recv()

            def panel(t, _):
                @pl.when(k > 0)
                def _():
                    recv(k - 1, t)
                    update(k - 1, t, sk)

                @pl.when((r != kr) & (t == t0))
                def _():
                    for b in range(3):
                        fb_copy(sk, b).wait_recv()
                solve(k, t, sk)
                each_send(k, t, lambda cp: cp.start())
                store(t, sk).start()
                return 0
            lax.fori_loop(t0, 8, panel, 0)

            @pl.when((r != kr) & (t0 >= 8))
            def _():
                for b in range(3):
                    fb_copy(sk, b).wait_recv()

            @pl.when(r == kr)
            def _():
                for b in range(3):
                    S[tk, SUB * b:SUB * (b + 1), pl.ds(pl.multiple_of(sk * BS + SUB * b, SUB), SUB)] = ub[b].T
                    for e in range(b + 1, 3):
                        S[tk, SUB * e:SUB * (e + 1), pl.ds(pl.multiple_of(sk * BS + SUB * b, SUB), SUB)] = FB[sk, b, :, SUB * e:SUB * (e + 1)].T
                        S[tk, SUB * b:SUB * (b + 1), pl.ds(pl.multiple_of(sk * BS + SUB * e, SUB), SUB)] = jnp.zeros((SUB, SUB), F32)
                store(tk, sk).start()

        @pl.when(k > 0)
        def _():
            @pl.when((c != kc) & (c != lax.rem(k + 3, 4)))
            def _():
                lax.fori_loop(t0, 8, lambda t, _: (recv(k - 1, t), 0)[1], 0)
            s0 = first_s(k)

            @pl.when(jnp.logical_not(same))
            def _():
                lax.fori_loop(s0, 4, lambda s, _: (q_local(k - 1, s).wait_recv(), 0)[1], 0)

            def bulk(n, _):
                t = t0 + n // 4
                s = lax.rem(n, 4)

                @pl.when((s >= s0) & lower(t, s))
                def _():
                    update(k - 1, t, s)
                return 0
            lax.fori_loop(0, 4 * (8 - t0), bulk, 0)
        return 0

    lax.fori_loop(0, NB, body, 0)

    def drain(k, _):
        t0 = first_t(k)
        own = c == lax.rem(k, 4)
        nxt = c == lax.rem(k + 1, 4)

        def one(t, _):
            @pl.when(own | nxt | (2 * t + r > k + 1))
            def _():
                each_send(k, t, lambda cp: cp.wait_send())
            return 0
        lax.fori_loop(t0, 8, one, 0)

        @pl.when(own & (r == lax.rem(k, 2)))
        def _():
            for b in range(3):
                fb_copy(k // 4, b).wait_send()
        return 0
    lax.fori_loop(0, NB, drain, 0)
    all_blocks(lambda t, s: store(t, s).wait())


def solution(mesh):
    def local(a):
        return pl.pallas_call(
            kernel,
            out_shape=jax.ShapeDtypeStruct(a.shape, F32),
            in_specs=[pl.BlockSpec(memory_space=pl.ANY)],
            out_specs=pl.BlockSpec(memory_space=pl.ANY),
            scratch_shapes=[
                pltpu.VMEM((8, BS, 4 * BS), F32),
                pltpu.VMEM((104, BS, BS), BF16),
                pltpu.VMEM((4, 3, SUB, BS), F32),
                pltpu.VMEM((BS, BS), F32),
                pltpu.VMEM((3, SUB, SUB), F32),
                pltpu.VMEM((SUB, SUB), F32),
                pltpu.VMEM((320, SUB), F32),
                pltpu.SemaphoreType.DMA((8, 4)),
                pltpu.SemaphoreType.DMA((8, 4)),
                pltpu.SemaphoreType.DMA((3, 64)),
                pltpu.SemaphoreType.DMA((64,)),
                pltpu.SemaphoreType.DMA((40,)),
                pltpu.SemaphoreType.DMA((4, 3)),
                pltpu.SemaphoreType.DMA((4, 3)),
            ],
            compiler_params=pltpu.CompilerParams(collective_id=0, has_side_effects=True,
                                                 vmem_limit_bytes=67043328),
            name="cholesky",
        )(a)

    spec = P(("batch", "row"), None, "col")
    return jax.shard_map(local, mesh=mesh, in_specs=(spec,), out_specs=spec, check_vma=False)
```

```python
import functools
import jax
import jax.numpy as jnp
from jax import lax
from jax.experimental import pallas as pl
from jax.experimental.pallas import tpu as pltpu
from jax.sharding import PartitionSpec as P

F32 = jnp.float32
BF16 = jnp.bfloat16
NB = 16
BS = 384
SUB = 128
MU = 4
LAG = MU - 1
HOP = MU // 2
MESH = pl.DeviceIdType.MESH


def dot_hi(a, b, dims):
    return lax.dot_general(a, b, (dims, ((), ())), precision=lax.Precision.HIGHEST, preferred_element_type=F32)


def lane_splat(x, i):
    return jnp.broadcast_to(x[:, i:i + 1], (8, SUB))


def row_splat(ref, row):
    return jnp.broadcast_to(ref[row:row + 1, :], (8, SUB))


def factor_tile(d_ref, off, u_ref, w_ref, sc):
    lane = lax.broadcasted_iota(jnp.int32, (8, SUB), 1)
    sub = lax.broadcasted_iota(jnp.int32, (8, SUB), 0)
    n_oct = SUB // 8
    X = [d_ref[pl.ds(pl.multiple_of(off + 8 * t, 8), 8), pl.ds(off, SUB)] for t in range(n_oct)]
    nxt = [lane_splat(X[0], i) for i in range(8)]
    for t in range(n_oct):
        j = 8 * t
        o = 160 * (t % 2)
        rows = X[t]
        for i in range(8):
            sc[o + 8 * i:o + 8 * i + 8, :] = nxt[i]
        d = {(m, i): row_splat(sc, o + 8 * i + m) for i in range(8) for m in range(i, 8)}
        sc[o + 64:o + 72, :] = rows
        sc[o + 72:o + 80, :] = jnp.where(lane < j, rows, jnp.where(lane == sub + j, 1.0, 0.0))
        inv = [None] * 8
        low = {}
        for i in range(8):
            inv[i] = lax.rsqrt(d[i, i])
            for m in range(i + 1, 8):
                low[m, i] = d[m, i] * inv[i]
            for m in range(i + 1, 8):
                for n in range(i + 1, m + 1):
                    d[m, n] = d[m, n] - low[m, i] * low[n, i]

        def column(s):
            c = []
            for i in range(8):
                x = lane_splat(X[s], j + i)
                for p in range(i):
                    x = x - low[i, p] * c[p]
                c.append(x * inv[i])
            return c

        if t + 1 < n_oct:
            first = column(t + 1)
            nxt = [lane_splat(X[t + 1], j + 8 + m) for m in range(8)]
            for i in range(8):
                sc[o + 80 + 8 * i:o + 88 + 8 * i, :] = first[i]
            for i in range(8):
                for m in range(8):
                    nxt[m] = nxt[m] - first[i] * row_splat(sc, o + 80 + 8 * i + m)
        u = []
        w = []
        for i in range(8):
            x = row_splat(sc, o + 64 + i)
            y = row_splat(sc, o + 72 + i)
            for p in range(i):
                x = x - low[i, p] * u[p]
                y = y - low[i, p] * w[p]
            u.append(x * inv[i])
            w.append(y * inv[i])
        u8 = u[7]
        w8 = w[7]
        for i in range(7):
            u8 = jnp.where(sub == i, u[i], u8)
            w8 = jnp.where(sub == i, w[i], w8)
        u_ref[j:j + 8, :] = jnp.where(lane >= sub + j, u8, 0.0)
        w_ref[j:j + 8, :] = jnp.where(lane < j + 8, w8, 0.0)
        z = [jnp.where(lane < j + 8, w[i], u[i]) for i in range(8)]
        for s in range(t + 1, n_oct):
            c = first if s == t + 1 else column(s)
            x = jnp.where((lane >= j) & (lane < j + 8), 0.0, X[s])
            for i in range(8):
                x = x - c[i] * z[i]
            X[s] = x


def kernel(a_hbm, o_hbm, S, PQ, FB, D, ub, wb, sc, ld_sem, st_sem, send_sem, p_sem, q_sem, fs_sem, fr_sem, us_sem, ur_sem):
    g = lax.axis_index("batch")
    r = lax.axis_index("row")
    c = lax.axis_index("col")
    n_q0 = 64
    same = r == lax.rem(c, 2)

    def blk(s):
        return pl.ds(pl.multiple_of(s * BS, SUB), BS)

    def p_idx(k, t):
        return 8 * k - (k // 2) * ((k + 1) // 2) + t - (k + 1) // 2

    def q_idx(k, s):
        m = k // 4
        return 4 * k - (4 * (m * (m - 1) // 2) + (k - 4 * m) * m) + s - m

    def first_t(k):
        return (k + 2 - r) // 2

    def to(row, col):
        return (g, row, col)

    def p_copy(k, t, kind, col):
        i = p_idx(k, t)
        return pltpu.make_async_remote_copy(PQ.at[i], PQ.at[i], send_sem.at[kind, i], p_sem.at[i],
                                            device_id=to(r, col), device_id_type=MESH)

    def q_copy(k, t):
        i = p_idx(k, t)
        j = 2 * t + r
        q = q_idx(k, j // 4)
        return pltpu.make_async_remote_copy(PQ.at[i], PQ.at[n_q0 + q], send_sem.at[2, i], q_sem.at[q],
                                            device_id=to(1 - r, lax.rem(j, 4)), device_id_type=MESH)

    def p_local(k, t):
        i = p_idx(k, t)
        return pltpu.make_async_remote_copy(PQ.at[i], PQ.at[i], send_sem.at[0, i], p_sem.at[i],
                                            device_id=to(r, c ^ 1), device_id_type=MESH)

    def q_local(k, s):
        q = q_idx(k, s)
        return pltpu.make_async_remote_copy(PQ.at[n_q0 + q], PQ.at[n_q0 + q], send_sem.at[2, 0], q_sem.at[q],
                                            device_id=to(1 - r, c), device_id_type=MESH)

    def each_send(k, t, act):
        kc = lax.rem(k, 4)
        far = 2 * t + r > k + 1
        own = c == kc

        @pl.when(own & far)
        def _():
            act(p_copy(k, t, 1, c ^ 3))
            act(p_copy(k, t, 0, c ^ 1))

        @pl.when(own)
        def _():
            act(q_copy(k, t))

        @pl.when((c == (kc ^ 3)) & far)
        def _():
            act(p_copy(k, t, 0, c ^ 1))

    def near_copy(k, n):
        view = PQ.at[p_idx(k, (k + 1) // 2), :, SUB * n:SUB * (n + 1)]
        return pltpu.make_async_remote_copy(view, view, us_sem.at[k, n], ur_sem.at[k, n],
                                            device_id=to(r, lax.rem(k + 1, 4)), device_id_type=MESH)

    def near_local(k, n):
        view = PQ.at[p_idx(k, (k + 1) // 2), :, SUB * n:SUB * (n + 1)]
        return pltpu.make_async_remote_copy(view, view, us_sem.at[k, n], ur_sem.at[k, n],
                                            device_id=to(r, lax.rem(k, 4)), device_id_type=MESH)

    def recv(k, t):
        p_local(k, t).wait_recv()

    def forward(k, t):
        recv(k, t)
        p_copy(k, t, 0, c ^ 1).start()

    def col_index(k, s):
        return jnp.where(same, p_idx(k, 2 * s + (c - r) // 2), n_q0 + q_idx(k, s))

    def update(k, t, s):
        @pl.when(k == 0)
        def _():
            load(t, s).wait()
        prod = lax.dot_general(PQ[p_idx(k, t)], PQ[col_index(k, s)], (((1,), (1,)), ((), ())),
                               preferred_element_type=F32)
        S[t, :, blk(s)] = S[t, :, blk(s)] - prod

    def fb_copy(slot, b):
        view = FB.at[slot, b, :, SUB * b:BS]
        return pltpu.make_async_remote_copy(view, view, fs_sem.at[slot, b], fr_sem.at[slot, b],
                                            device_id=to(1 - r, c), device_id_type=MESH)

    def load(t, s):
        return pltpu.make_async_copy(a_hbm.at[t, :, blk(s)], S.at[t, :, blk(s)], ld_sem.at[t, s])

    def store(t, s):
        return pltpu.make_async_copy(S.at[t, :, blk(s)], o_hbm.at[t, :, blk(s)], st_sem.at[t, s])

    def lower(t, s):
        return 2 * t + r >= 4 * s + c

    def all_blocks(fn):
        def body(n, _):
            fn(lax.rem(n, 8), n // 8)
            return 0
        lax.fori_loop(0, 32, body, 0)

    def begin(t, s):
        @pl.when(lower(t, s))
        def _():
            load(t, s).start()

    def blank_copy(t, s):
        return pltpu.make_async_copy(S.at[0, :, 3 * BS:4 * BS], o_hbm.at[t, :, blk(s)], st_sem.at[t, s])

    def blank(t, s):
        @pl.when(jnp.logical_not(lower(t, s)))
        def _():
            blank_copy(t, s).start()

    barrier = pltpu.get_barrier_semaphore()
    all_blocks(begin)
    for step in range(1, 8):
        dr, dc = step // 4, step % 4
        pl.semaphore_signal(barrier, inc=1, device_id=to(r ^ dr, c ^ dc), device_id_type=MESH)
    S[0, :, 3 * BS:4 * BS] = jnp.zeros((BS, BS), F32)
    pl.semaphore_wait(barrier, 7)

    def factor_diag(slot, more):
        def tile(b, _):
            off = pl.multiple_of(b * SUB, SUB)
            factor_tile(D, off, ub.at[b], wb, sc)
            w = wb[...]
            FB[slot, b, :, pl.ds(off, SUB)] = w

            @pl.when(b == 0)
            def _():
                rest = dot_hi(w, D[0:SUB, SUB:BS], ((1,), (0,)))
                FB[slot, 0, :, SUB:BS] = rest
                @pl.when(more)
                def _():
                    fb_copy(slot, 0).start()
                D[SUB:BS, SUB:BS] = D[SUB:BS, SUB:BS] - dot_hi(rest, rest, ((0,), (0,)))

            @pl.when(b == 1)
            def _():
                rest = dot_hi(w, D[SUB:2 * SUB, 2 * SUB:BS], ((1,), (0,)))
                FB[slot, 1, :, 2 * SUB:BS] = rest
                @pl.when(more)
                def _():
                    fb_copy(slot, 1).start()
                D[2 * SUB:BS, 2 * SUB:BS] = D[2 * SUB:BS, 2 * SUB:BS] - dot_hi(rest, rest, ((0,), (0,)))

            @pl.when(b == 2)
            def _():
                @pl.when(more)
                def _():
                    fb_copy(slot, 2).start()
            return 0
        lax.fori_loop(0, 3, tile, 0)

    def solve(k, t, s, ready, done):
        idx = p_idx(k, t)

        def tile(n):
            return pl.ds(pl.multiple_of(s * BS + SUB * n, SUB), SUB)

        def put(n, x):
            PQ[idx, :, SUB * n:SUB * (n + 1)] = x.astype(BF16)
            S[t, :, tile(n)] = x
            done(n)

        ready(0)
        x1 = dot_hi(S[t, :, tile(0)], FB[s, 0, :, 0:SUB], ((1,), (1,)))
        put(0, x1)
        rest = S[t, :, pl.ds(pl.multiple_of(s * BS + SUB, SUB), 2 * SUB)] - dot_hi(x1, FB[s, 0, :, SUB:BS], ((1,), (0,)))
        ready(1)
        x2 = dot_hi(rest[:, 0:SUB], FB[s, 1, :, SUB:2 * SUB], ((1,), (1,)))
        put(1, x2)
        last = rest[:, SUB:2 * SUB] - dot_hi(x2, FB[s, 1, :, 2 * SUB:BS], ((1,), (0,)))
        ready(2)
        put(2, dot_hi(last, FB[s, 2, :, 2 * SUB:BS], ((1,), (1,))))

    def wave(n, _):
        kd = n // MU
        sd = kd // 4
        td = kd // 2
        diag = (lax.rem(n, MU) == 0) & (c == lax.rem(kd, 4)) & (r == lax.rem(kd, 2))

        @pl.when(diag)
        def _():
            @pl.when(kd > 0)
            def _():
                @pl.when(kd == 1)
                def _():
                    load(td, sd).wait()
                D[...] = S[td, :, blk(sd)]
                idx = p_idx(kd - 1, td)
                for e in range(3):
                    near_local(kd - 1, e).wait_recv()
                    part = PQ[idx, :, SUB * e:SUB * (e + 1)]
                    D[...] = D[...] - lax.dot_general(part, part, (((1,), (1,)), ((), ())), preferred_element_type=F32)

            @pl.when(kd == 0)
            def _():
                load(td, sd).wait()
                D[...] = S[td, :, blk(sd)]
            factor_diag(sd, kd < NB - 1)

        near = (lax.rem(n, MU) == 1) & (c == lax.rem(kd, 4)) & (r == lax.rem(kd + 1, 2))

        @pl.when(near)
        def _():
            t = (kd + 1) // 2

            @pl.when(kd == 0)
            def _():
                load(t, sd).wait()

            @pl.when(kd > 0)
            def _():
                @pl.when(lax.rem(kd, 2) == 1)
                def _():
                    recv(kd - 1, t)
                update(kd - 1, t, sd)
            solve(kd, t, sd, lambda e: fb_copy(sd, e).wait_recv(), lambda e: near_copy(kd, e).start())
            each_send(kd, t, lambda cp: cp.start())
            store(t, sd).start()

        def span(v):
            par = lax.rem(v + r, 2)
            lo = (jnp.maximum(v - (NB - 1) + LAG - 1, 0) // LAG + 1 - par) // 2
            hi = ((v + MU - 2) // MU + 1 - par) // 2
            return par, lo, hi

        @pl.when(n >= HOP)
        def _():
            v = n - HOP
            par, lo, hi = span(v)

            def pass_on(m, _):
                k = 2 * m + par

                @pl.when(c == (lax.rem(k, 4) ^ 3))
                def _():
                    forward(k, (v - LAG * k - r) // 2)
                return 0
            lax.fori_loop(lo, hi, pass_on, 0)

        @pl.when(n >= LAG)
        def _():
            v = n - LAG
            par, lo, hi = span(v)
            hi = hi - jnp.where(near & (kd > 0), 1, 0)

            def arrive(m, _):
                k = 2 * m + par
                kc = lax.rem(k, 4)

                @pl.when((c != kc) & (c != (kc ^ 3)))
                def _():
                    recv(k, (v - LAG * k - r) // 2)
                return 0
            lax.fori_loop(lo, hi, arrive, 0)

            @pl.when(jnp.logical_not(same))
            def _():
                def arrive_q(s, _):
                    j = 4 * s + c
                    d = v - j

                    @pl.when((d >= 0) & (lax.rem(d, LAG) == 0) & (d < LAG * j))
                    def _():
                        q_local(d // LAG, s).wait_recv()
                    return 0
                lax.fori_loop(0, 4, arrive_q, 0)

            def apply(m, _):
                k = 2 * m + par
                i = v - LAG * k

                def one(s, _):
                    update(k, (i - r) // 2, s)
                    return 0
                lax.fori_loop((k + 4 - c) // 4, (i + 4 - c) // 4, one, 0)
                return 0
            lax.fori_loop(lo, hi, apply, 0)

        @pl.when(lax.rem(n + c, 2) == r)
        def _():
            def task(m, _):
                s = 3 - m
                k = 4 * s + c
                i = n - LAG * k

                @pl.when((i > k + 1) & (i < NB))
                def _():
                    t = (i - r) // 2

                    @pl.when(k == 0)
                    def _():
                        load(t, s).wait()
                    solve(k, t, s, lambda e: None, lambda e: None)
                    each_send(k, t, lambda cp: cp.start())
                    store(t, s).start()
                return 0
            lax.fori_loop(0, 4, task, 0)

        @pl.when(diag)
        def _():
            for b in range(3):
                S[td, SUB * b:SUB * (b + 1), pl.ds(pl.multiple_of(sd * BS + SUB * b, SUB), SUB)] = ub[b].T
                for e in range(b + 1, 3):
                    S[td, SUB * e:SUB * (e + 1), pl.ds(pl.multiple_of(sd * BS + SUB * b, SUB), SUB)] = FB[sd, b, :, SUB * e:SUB * (e + 1)].T
                    S[td, SUB * b:SUB * (b + 1), pl.ds(pl.multiple_of(sd * BS + SUB * e, SUB), SUB)] = jnp.zeros((SUB, SUB), F32)
            store(td, sd).start()

        @pl.when(n == 1)
        def _():
            all_blocks(blank)
        return 0

    lax.fori_loop(0, MU * (NB - 1) + 1, wave, 0)

    def drain(k, _):
        t0 = first_t(k)
        own = c == lax.rem(k, 4)

        def one(t, _):
            each_send(k, t, lambda cp: cp.wait_send())
            return 0
        lax.fori_loop(t0, 8, one, 0)

        @pl.when(own & (k < NB - 1))
        def _():
            @pl.when(r == lax.rem(k, 2))
            def _():
                for b in range(3):
                    fb_copy(k // 4, b).wait_send()

            @pl.when(r != lax.rem(k, 2))
            def _():
                for b in range(3):
                    near_copy(k, b).wait_send()
        return 0
    lax.fori_loop(0, NB, drain, 0)
    all_blocks(lambda t, s: store(t, s).wait())


def solution(mesh):
    def local(a):
        return pl.pallas_call(
            kernel,
            out_shape=jax.ShapeDtypeStruct(a.shape, F32),
            in_specs=[pl.BlockSpec(memory_space=pl.ANY)],
            out_specs=pl.BlockSpec(memory_space=pl.ANY),
            scratch_shapes=[
                pltpu.VMEM((8, BS, 4 * BS), F32),
                pltpu.VMEM((104, BS, BS), BF16),
                pltpu.VMEM((4, 3, SUB, BS), F32),
                pltpu.VMEM((BS, BS), F32),
                pltpu.VMEM((3, SUB, SUB), F32),
                pltpu.VMEM((SUB, SUB), F32),
                pltpu.VMEM((320, SUB), F32),
                pltpu.SemaphoreType.DMA((8, 4)),
                pltpu.SemaphoreType.DMA((8, 4)),
                pltpu.SemaphoreType.DMA((3, 64)),
                pltpu.SemaphoreType.DMA((64,)),
                pltpu.SemaphoreType.DMA((40,)),
                pltpu.SemaphoreType.DMA((4, 3)),
                pltpu.SemaphoreType.DMA((4, 3)),
                pltpu.SemaphoreType.DMA((16, 3)),
                pltpu.SemaphoreType.DMA((16, 3)),
            ],
            compiler_params=pltpu.CompilerParams(collective_id=0, has_side_effects=True,
                                                 vmem_limit_bytes=67043328),
            name="cholesky",
        )(a)

    spec = P(("batch", "row"), None, "col")
    return jax.shard_map(local, mesh=mesh, in_specs=(spec,), out_specs=spec, check_vma=False)
```

```python
import functools
import jax
import jax.numpy as jnp
from jax import lax
from jax.experimental import pallas as pl
from jax.experimental.pallas import tpu as pltpu
from jax.sharding import PartitionSpec as P

F32 = jnp.float32
BF16 = jnp.bfloat16
NB = 16
BS = 384
SUB = 128
MU = 4
LAG = MU - 1
HOP = MU // 2
LAST = NB - 1
MESH = pl.DeviceIdType.MESH


def dot_hi(a, b, dims):
    return lax.dot_general(a, b, (dims, ((), ())), precision=lax.Precision.HIGHEST, preferred_element_type=F32)


def lane_splat(x, i):
    return jnp.broadcast_to(x[:, i:i + 1], (8, SUB))


def row_splat(ref, row):
    return jnp.broadcast_to(ref[row:row + 1, :], (8, SUB))


def factor_tile(d_ref, off, u_ref, w_ref, sc):
    lane = lax.broadcasted_iota(jnp.int32, (8, SUB), 1)
    sub = lax.broadcasted_iota(jnp.int32, (8, SUB), 0)
    n_oct = SUB // 8
    half = n_oct // 2
    X = [d_ref[pl.ds(pl.multiple_of(off + 8 * t, 8), 8), pl.ds(off, SUB)] for t in range(n_oct)]
    nxt = [lane_splat(X[0], i) for i in range(8)]
    for t in range(n_oct):
        j = 8 * t
        o = 160 * (t % 2)
        rows = X[t]
        for i in range(8):
            sc[o + 8 * i:o + 8 * i + 8, :] = nxt[i]
        d = {(m, i): row_splat(sc, o + 8 * i + m) for i in range(8) for m in range(i, 8)}
        sc[o + 64:o + 72, :] = rows
        sc[o + 72:o + 80, :] = jnp.where(lane < j, rows, jnp.where(lane == sub + j, 1.0, 0.0))
        inv = [None] * 8
        low = {}
        for i in range(8):
            inv[i] = lax.rsqrt(d[i, i])
            for m in range(i + 1, 8):
                low[m, i] = d[m, i] * inv[i]
            for m in range(i + 1, 8):
                for n in range(i + 1, m + 1):
                    d[m, n] = d[m, n] - low[m, i] * low[n, i]

        def column(s):
            c = []
            for i in range(8):
                x = lane_splat(X[s], j + i)
                for p in range(i):
                    x = x - low[i, p] * c[p]
                c.append(x * inv[i])
            return c

        end = (t // half + 1) * half
        if t + 1 < end:
            first = column(t + 1)
            nxt = [lane_splat(X[t + 1], j + 8 + m) for m in range(8)]
            for i in range(8):
                sc[o + 80 + 8 * i:o + 88 + 8 * i, :] = first[i]
            for i in range(8):
                for m in range(8):
                    nxt[m] = nxt[m] - first[i] * row_splat(sc, o + 80 + 8 * i + m)
        u = []
        w = []
        for i in range(8):
            x = row_splat(sc, o + 64 + i)
            y = row_splat(sc, o + 72 + i)
            for p in range(i):
                x = x - low[i, p] * u[p]
                y = y - low[i, p] * w[p]
            u.append(x * inv[i])
            w.append(y * inv[i])
        u8 = u[7]
        w8 = w[7]
        for i in range(7):
            u8 = jnp.where(sub == i, u[i], u8)
            w8 = jnp.where(sub == i, w[i], w8)
        u_ref[j:j + 8, :] = jnp.where(lane >= sub + j, u8, 0.0)
        w_ref[j:j + 8, :] = jnp.where(lane < j + 8, w8, 0.0)
        z = [jnp.where(lane < j + 8, w[i], u[i]) for i in range(8)]
        for s in range(t + 1, end):
            c = first if s == t + 1 else column(s)
            x = jnp.where((lane >= j) & (lane < j + 8), 0.0, X[s])
            for i in range(8):
                x = x - c[i] * z[i]
            X[s] = x
        if t + 1 == half:
            e = 8 * half
            top = u_ref[0:e, :]
            z = jnp.where(lax.broadcasted_iota(jnp.int32, (e, SUB), 1) < e, w_ref[0:e, :], top)
            prod = dot_hi(top[:, e:SUB], z, ((0,), (0,)))
            for s in range(half, n_oct):
                X[s] = jnp.where(lane < e, 0.0, X[s]) - prod[8 * (s - half):8 * (s - half + 1), :]
            nxt = [lane_splat(X[half], e + m) for m in range(8)]


def kernel(a_hbm, o_hbm, S, PQ, FB, D, ub, wb, sc, ld_sem, st_sem, send_sem, p_sem, q_sem, fs_sem, fr_sem, us_sem, ur_sem):
    g = lax.axis_index("batch")
    r = lax.axis_index("row")
    c = lax.axis_index("col")
    n_q0 = 64
    same = r == lax.rem(c, 2)

    def blk(s):
        return pl.ds(pl.multiple_of(s * BS, SUB), BS)

    def p_idx(k, t):
        return 8 * k - (k // 2) * ((k + 1) // 2) + t - (k + 1) // 2

    def q_idx(k, s):
        m = k // 4
        return 4 * k - (4 * (m * (m - 1) // 2) + (k - 4 * m) * m) + s - m

    def first_t(k):
        return (k + 2 - r) // 2

    def to(row, col):
        return (g, row, col)

    def across(k):
        kc = lax.rem(k, 4)
        return jnp.where(lax.rem(kc, 2) == r, kc ^ 3, kc ^ 2)

    def p_copy(k, t, kind, col):
        i = p_idx(k, t)
        return pltpu.make_async_remote_copy(PQ.at[i], PQ.at[i], send_sem.at[kind, i], p_sem.at[i],
                                            device_id=to(r, col), device_id_type=MESH)

    def q_copy(k, t):
        i = p_idx(k, t)
        j = 2 * t + r
        q = q_idx(k, j // 4)
        return pltpu.make_async_remote_copy(PQ.at[i], PQ.at[n_q0 + q], send_sem.at[2, i], q_sem.at[q],
                                            device_id=to(1 - r, lax.rem(j, 4)), device_id_type=MESH)

    def p_local(k, t):
        i = p_idx(k, t)
        return pltpu.make_async_remote_copy(PQ.at[i], PQ.at[i], send_sem.at[0, i], p_sem.at[i],
                                            device_id=to(r, c ^ 1), device_id_type=MESH)

    def q_local(k, s):
        q = q_idx(k, s)
        return pltpu.make_async_remote_copy(PQ.at[n_q0 + q], PQ.at[n_q0 + q], send_sem.at[2, 0], q_sem.at[q],
                                            device_id=to(1 - r, c), device_id_type=MESH)

    def each_send(k, t, act):
        kc = lax.rem(k, 4)
        i = 2 * t + r
        j = lax.rem(i, 4)
        far = i > k + 1
        own = c == kc

        @pl.when(own & far)
        def _():
            act(p_copy(k, t, 1, across(k)))
            act(p_copy(k, t, 0, c ^ 1))

        @pl.when(own & (i < LAST) & (jnp.logical_not(far) | (j // 2 == kc // 2)))
        def _():
            act(q_copy(k, t))

        @pl.when((c == across(k)) & far)
        def _():
            act(p_copy(k, t, 0, c ^ 1))

            @pl.when((i < LAST) & (j == (c ^ 1)))
            def _():
                act(q_copy(k, t))

    def near_copy(k, n):
        view = PQ.at[p_idx(k, (k + 1) // 2), :, SUB * n:SUB * (n + 1)]
        return pltpu.make_async_remote_copy(view, view, us_sem.at[k, n], ur_sem.at[k, n],
                                            device_id=to(r, lax.rem(k + 1, 4)), device_id_type=MESH)

    def near_local(k, n):
        view = PQ.at[p_idx(k, (k + 1) // 2), :, SUB * n:SUB * (n + 1)]
        return pltpu.make_async_remote_copy(view, view, us_sem.at[k, n], ur_sem.at[k, n],
                                            device_id=to(r, lax.rem(k, 4)), device_id_type=MESH)

    def recv(k, t):
        p_local(k, t).wait_recv()

    def forward(k, t):
        recv(k, t)
        each_send(k, t, lambda cp: cp.start())

    def col_index(k, s):
        return jnp.where(same, p_idx(k, 2 * s + (c - r) // 2), n_q0 + q_idx(k, s))

    def update(k, t, s):
        @pl.when(k == 0)
        def _():
            load(t, s).wait()
        prod = lax.dot_general(PQ[p_idx(k, t)], PQ[col_index(k, s)], (((1,), (1,)), ((), ())),
                               preferred_element_type=F32)
        S[t, :, blk(s)] = S[t, :, blk(s)] - prod

    def fb_copy(slot, b):
        view = FB.at[slot, b, :, SUB * b:BS]
        return pltpu.make_async_remote_copy(view, view, fs_sem.at[slot, b], fr_sem.at[slot, b],
                                            device_id=to(1 - r, c), device_id_type=MESH)

    def load(t, s):
        return pltpu.make_async_copy(a_hbm.at[t, :, blk(s)], S.at[t, :, blk(s)], ld_sem.at[t, s])

    def store(t, s):
        return pltpu.make_async_copy(S.at[t, :, blk(s)], o_hbm.at[t, :, blk(s)], st_sem.at[t, s])

    def lower(t, s):
        return 2 * t + r >= 4 * s + c

    def all_blocks(fn):
        def body(n, _):
            fn(lax.rem(n, 8), n // 8)
            return 0
        lax.fori_loop(0, 32, body, 0)

    def begin(t, s):
        @pl.when(lower(t, s))
        def _():
            load(t, s).start()

    def blank_copy(t, s):
        return pltpu.make_async_copy(S.at[0, :, 3 * BS:4 * BS], o_hbm.at[t, :, blk(s)], st_sem.at[t, s])

    def blank(t, s):
        @pl.when(jnp.logical_not(lower(t, s)))
        def _():
            blank_copy(t, s).start()

    barrier = pltpu.get_barrier_semaphore()
    all_blocks(begin)
    for step in range(1, 8):
        dr, dc = step // 4, step % 4
        pl.semaphore_signal(barrier, inc=1, device_id=to(r ^ dr, c ^ dc), device_id_type=MESH)
    S[0, :, 3 * BS:4 * BS] = jnp.zeros((BS, BS), F32)
    pl.semaphore_wait(barrier, 7)

    def factor_diag(slot, more):
        def tile(b, _):
            off = pl.multiple_of(b * SUB, SUB)
            factor_tile(D, off, ub.at[b], wb, sc)
            w = wb[...]
            FB[slot, b, :, pl.ds(off, SUB)] = w

            @pl.when(b == 0)
            def _():
                rest = dot_hi(w, D[0:SUB, SUB:BS], ((1,), (0,)))
                FB[slot, 0, :, SUB:BS] = rest
                @pl.when(more)
                def _():
                    fb_copy(slot, 0).start()
                D[SUB:BS, SUB:BS] = D[SUB:BS, SUB:BS] - dot_hi(rest, rest, ((0,), (0,)))

            @pl.when(b == 1)
            def _():
                rest = dot_hi(w, D[SUB:2 * SUB, 2 * SUB:BS], ((1,), (0,)))
                FB[slot, 1, :, 2 * SUB:BS] = rest
                @pl.when(more)
                def _():
                    fb_copy(slot, 1).start()
                D[2 * SUB:BS, 2 * SUB:BS] = D[2 * SUB:BS, 2 * SUB:BS] - dot_hi(rest, rest, ((0,), (0,)))

            @pl.when(b == 2)
            def _():
                @pl.when(more)
                def _():
                    fb_copy(slot, 2).start()
            return 0
        lax.fori_loop(0, 3, tile, 0)

    def solve(k, t, s, ready, done):
        idx = p_idx(k, t)

        def tile(n):
            return pl.ds(pl.multiple_of(s * BS + SUB * n, SUB), SUB)

        def put(n, x):
            PQ[idx, :, SUB * n:SUB * (n + 1)] = x.astype(BF16)
            S[t, :, tile(n)] = x
            done(n)

        ready(0)
        x1 = dot_hi(S[t, :, tile(0)], FB[s, 0, :, 0:SUB], ((1,), (1,)))
        put(0, x1)
        rest = S[t, :, pl.ds(pl.multiple_of(s * BS + SUB, SUB), 2 * SUB)] - dot_hi(x1, FB[s, 0, :, SUB:BS], ((1,), (0,)))
        ready(1)
        x2 = dot_hi(rest[:, 0:SUB], FB[s, 1, :, SUB:2 * SUB], ((1,), (1,)))
        put(1, x2)
        last = rest[:, SUB:2 * SUB] - dot_hi(x2, FB[s, 1, :, 2 * SUB:BS], ((1,), (0,)))
        ready(2)
        put(2, dot_hi(last, FB[s, 2, :, 2 * SUB:BS], ((1,), (1,))))

    def wave(n, _):
        kd = n // MU
        sd = kd // 4
        td = kd // 2
        diag = (lax.rem(n, MU) == 0) & (c == lax.rem(kd, 4)) & (r == lax.rem(kd, 2))

        @pl.when(diag)
        def _():
            @pl.when(kd > 0)
            def _():
                @pl.when(kd == 1)
                def _():
                    load(td, sd).wait()
                D[...] = S[td, :, blk(sd)]
                idx = p_idx(kd - 1, td)
                for e in range(3):
                    near_local(kd - 1, e).wait_recv()
                    part = PQ[idx, :, SUB * e:SUB * (e + 1)]
                    D[...] = D[...] - lax.dot_general(part, part, (((1,), (1,)), ((), ())), preferred_element_type=F32)

            @pl.when(kd == 0)
            def _():
                load(td, sd).wait()
                D[...] = S[td, :, blk(sd)]
            factor_diag(sd, kd < NB - 1)

        def span(v):
            par = lax.rem(v + r, 2)
            lo = (jnp.maximum(v - (NB - 1) + LAG - 1, 0) // LAG + 1 - par) // 2
            hi = ((v + MU - 2) // MU + 1 - par) // 2
            return par, lo, hi

        @pl.when(n >= HOP)
        def _():
            v = n - HOP
            par, lo, hi = span(v)

            def pass_on(m, _):
                k = 2 * m + par

                @pl.when(c == across(k))
                def _():
                    forward(k, (v - LAG * k - r) // 2)
                return 0
            lax.fori_loop(lo, hi, pass_on, 0)

        near = (lax.rem(n, MU) == 1) & (c == lax.rem(kd, 4)) & (r == lax.rem(kd + 1, 2))

        @pl.when(near)
        def _():
            t = (kd + 1) // 2

            @pl.when(kd == 0)
            def _():
                load(t, sd).wait()

            @pl.when(kd > 0)
            def _():
                q_local(kd - 1, sd).wait_recv()

                @pl.when(lax.rem(kd, 2) == 1)
                def _():
                    recv(kd - 1, t)
                update(kd - 1, t, sd)
            solve(kd, t, sd, lambda e: fb_copy(sd, e).wait_recv(), lambda e: near_copy(kd, e).start())
            each_send(kd, t, lambda cp: cp.start())
            store(t, sd).start()

        @pl.when(n >= LAG)
        def _():
            v = n - LAG
            par, lo, hi = span(v)
            hi = hi - jnp.where(near & (kd > 0), 1, 0)

            def arrive(m, _):
                k = 2 * m + par

                @pl.when((c != lax.rem(k, 4)) & (c != across(k)))
                def _():
                    recv(k, (v - LAG * k - r) // 2)
                return 0
            lax.fori_loop(lo, hi, arrive, 0)

            @pl.when(jnp.logical_not(same))
            def _():
                def arrive_q(s, _):
                    j = 4 * s + c
                    d = v - 1 - j

                    @pl.when((j < LAST) & (d >= 0) & (lax.rem(d, LAG) == 0) & (d < LAG * (j - 1)))
                    def _():
                        q_local(d // LAG, s).wait_recv()
                    return 0
                lax.fori_loop(0, 4, arrive_q, 0)

            def apply(m, _):
                k = 2 * m + par
                i = v - LAG * k

                def one(s, _):
                    update(k, (i - r) // 2, s)
                    return 0
                lax.fori_loop((k + 4 - c) // 4, (i + 4 - c) // 4, one, 0)
                return 0
            lax.fori_loop(lo, hi, apply, 0)

        @pl.when(lax.rem(n + c, 2) == r)
        def _():
            def task(m, _):
                s = 3 - m
                k = 4 * s + c
                i = n - LAG * k

                @pl.when((i > k + 1) & (i < NB))
                def _():
                    t = (i - r) // 2

                    @pl.when(k == 0)
                    def _():
                        load(t, s).wait()
                    solve(k, t, s, lambda e: None, lambda e: None)
                    each_send(k, t, lambda cp: cp.start())
                    store(t, s).start()
                return 0
            lax.fori_loop(0, 4, task, 0)

        @pl.when(diag)
        def _():
            for b in range(3):
                S[td, SUB * b:SUB * (b + 1), pl.ds(pl.multiple_of(sd * BS + SUB * b, SUB), SUB)] = ub[b].T
                for e in range(b + 1, 3):
                    S[td, SUB * e:SUB * (e + 1), pl.ds(pl.multiple_of(sd * BS + SUB * b, SUB), SUB)] = FB[sd, b, :, SUB * e:SUB * (e + 1)].T
                    S[td, SUB * b:SUB * (b + 1), pl.ds(pl.multiple_of(sd * BS + SUB * e, SUB), SUB)] = jnp.zeros((SUB, SUB), F32)
            store(td, sd).start()

        @pl.when(n == 1)
        def _():
            all_blocks(blank)
        return 0

    lax.fori_loop(0, MU * (NB - 1) + 1, wave, 0)

    def drain(k, _):
        t0 = first_t(k)
        own = c == lax.rem(k, 4)

        def one(t, _):
            each_send(k, t, lambda cp: cp.wait_send())
            return 0
        lax.fori_loop(t0, 8, one, 0)

        @pl.when(own & (k < NB - 1))
        def _():
            @pl.when(r == lax.rem(k, 2))
            def _():
                for b in range(3):
                    fb_copy(k // 4, b).wait_send()

            @pl.when(r != lax.rem(k, 2))
            def _():
                for b in range(3):
                    near_copy(k, b).wait_send()
        return 0
    lax.fori_loop(0, NB, drain, 0)
    all_blocks(lambda t, s: store(t, s).wait())


def solution(mesh):
    def local(a):
        return pl.pallas_call(
            kernel,
            out_shape=jax.ShapeDtypeStruct(a.shape, F32),
            in_specs=[pl.BlockSpec(memory_space=pl.ANY)],
            out_specs=pl.BlockSpec(memory_space=pl.ANY),
            scratch_shapes=[
                pltpu.VMEM((8, BS, 4 * BS), F32),
                pltpu.VMEM((104, BS, BS), BF16),
                pltpu.VMEM((4, 3, SUB, BS), F32),
                pltpu.VMEM((BS, BS), F32),
                pltpu.VMEM((3, SUB, SUB), F32),
                pltpu.VMEM((SUB, SUB), F32),
                pltpu.VMEM((320, SUB), F32),
                pltpu.SemaphoreType.DMA((8, 4)),
                pltpu.SemaphoreType.DMA((8, 4)),
                pltpu.SemaphoreType.DMA((3, 64)),
                pltpu.SemaphoreType.DMA((64,)),
                pltpu.SemaphoreType.DMA((40,)),
                pltpu.SemaphoreType.DMA((4, 3)),
                pltpu.SemaphoreType.DMA((4, 3)),
                pltpu.SemaphoreType.DMA((16, 3)),
                pltpu.SemaphoreType.DMA((16, 3)),
            ],
            compiler_params=pltpu.CompilerParams(collective_id=0, has_side_effects=True,
                                                 vmem_limit_bytes=67043328),
            name="cholesky",
        )(a)

    spec = P(("batch", "row"), None, "col")
    return jax.shard_map(local, mesh=mesh, in_specs=(spec,), out_specs=spec, check_vma=False)
```

```python
import functools
import jax
import jax.numpy as jnp
from jax import lax
from jax.experimental import pallas as pl
from jax.experimental.pallas import tpu as pltpu
from jax.sharding import PartitionSpec as P

F32 = jnp.float32
BF16 = jnp.bfloat16
NB = 16
BS = 384
SUB = 128
MU = 4
LAG = MU - 1
HOP = MU // 2
LAST = NB - 1
MESH = pl.DeviceIdType.MESH


def dot_hi(a, b, dims):
    return lax.dot_general(a, b, (dims, ((), ())), precision=lax.Precision.HIGHEST, preferred_element_type=F32)


def lane_splat(x, i):
    return jnp.broadcast_to(x[:, i:i + 1], (8, SUB))


def row_splat(ref, row):
    return jnp.broadcast_to(ref[row:row + 1, :], (8, SUB))


def factor_tile(d_ref, off, u_ref, w_ref, sc):
    lane = lax.broadcasted_iota(jnp.int32, (8, SUB), 1)
    sub = lax.broadcasted_iota(jnp.int32, (8, SUB), 0)
    n_oct = SUB // 8
    half = n_oct // 2
    X = [d_ref[pl.ds(pl.multiple_of(off + 8 * t, 8), 8), pl.ds(off, SUB)] for t in range(n_oct)]
    nxt = [lane_splat(X[0], i) for i in range(8)]
    for t in range(n_oct):
        j = 8 * t
        o = 160 * (t % 2)
        rows = X[t]
        for i in range(8):
            sc[o + 8 * i:o + 8 * i + 8, :] = nxt[i]
        d = {(m, i): row_splat(sc, o + 8 * i + m) for i in range(8) for m in range(i, 8)}
        sc[o + 64:o + 72, :] = rows
        sc[o + 72:o + 80, :] = jnp.where(lane < j, rows, jnp.where(lane == sub + j, 1.0, 0.0))
        inv = [None] * 8
        low = {}
        for i in range(8):
            inv[i] = lax.rsqrt(d[i, i])
            for m in range(i + 1, 8):
                low[m, i] = d[m, i] * inv[i]
            for m in range(i + 1, 8):
                for n in range(i + 1, m + 1):
                    d[m, n] = d[m, n] - low[m, i] * low[n, i]

        def column(s):
            c = []
            for i in range(8):
                x = lane_splat(X[s], j + i)
                for p in range(i):
                    x = x - low[i, p] * c[p]
                c.append(x * inv[i])
            return c

        end = (t // half + 1) * half
        if t + 1 < end:
            first = column(t + 1)
            nxt = [lane_splat(X[t + 1], j + 8 + m) for m in range(8)]
            for i in range(8):
                sc[o + 80 + 8 * i:o + 88 + 8 * i, :] = first[i]
            for i in range(8):
                for m in range(8):
                    nxt[m] = nxt[m] - first[i] * row_splat(sc, o + 80 + 8 * i + m)
        u = []
        w = []
        for i in range(8):
            x = row_splat(sc, o + 64 + i)
            y = row_splat(sc, o + 72 + i)
            for p in range(i):
                x = x - low[i, p] * u[p]
                y = y - low[i, p] * w[p]
            u.append(x * inv[i])
            w.append(y * inv[i])
        u8 = u[7]
        w8 = w[7]
        for i in range(7):
            u8 = jnp.where(sub == i, u[i], u8)
            w8 = jnp.where(sub == i, w[i], w8)
        u_ref[j:j + 8, :] = jnp.where(lane >= sub + j, u8, 0.0)
        w_ref[j:j + 8, :] = jnp.where(lane < j + 8, w8, 0.0)
        z = [jnp.where(lane < j + 8, w[i], u[i]) for i in range(8)]
        for s in range(t + 1, end):
            c = first if s == t + 1 else column(s)
            x = jnp.where((lane >= j) & (lane < j + 8), 0.0, X[s])
            for i in range(8):
                x = x - c[i] * z[i]
            X[s] = x
        if t + 1 == half:
            e = 8 * half
            top = u_ref[0:e, :]
            z = jnp.where(lax.broadcasted_iota(jnp.int32, (e, SUB), 1) < e, w_ref[0:e, :], top)
            prod = dot_hi(top[:, e:SUB], z, ((0,), (0,)))
            for s in range(half, n_oct):
                X[s] = jnp.where(lane < e, 0.0, X[s]) - prod[8 * (s - half):8 * (s - half + 1), :]
            nxt = [lane_splat(X[half], e + m) for m in range(8)]


def kernel(a_hbm, o_hbm, S, PQ, FB, D, ub, wb, sc, ld_sem, st_sem, send_sem, p_sem, q_sem, fs_sem, fr_sem, us_sem, ur_sem):
    g = lax.axis_index("batch")
    r = lax.axis_index("row")
    c = lax.axis_index("col")
    n_q0 = 64
    same = r == lax.rem(c, 2)

    def blk(s):
        return pl.ds(pl.multiple_of(s * BS, SUB), BS)

    def p_idx(k, t):
        return 8 * k - (k // 2) * ((k + 1) // 2) + t - (k + 1) // 2

    def q_idx(k, s):
        m = k // 4
        return 4 * k - (4 * (m * (m - 1) // 2) + (k - 4 * m) * m) + s - m

    def first_t(k):
        return (k + 2 - r) // 2

    def to(row, col):
        return (g, row, col)

    def across(k):
        kc = lax.rem(k, 4)
        return jnp.where(lax.rem(kc, 2) == r, kc ^ 3, kc ^ 2)

    def p_copy(k, t, kind, col):
        i = p_idx(k, t)
        return pltpu.make_async_remote_copy(PQ.at[i], PQ.at[i], send_sem.at[kind, i], p_sem.at[i],
                                            device_id=to(r, col), device_id_type=MESH)

    def q_copy(k, t):
        i = p_idx(k, t)
        j = 2 * t + r
        q = q_idx(k, j // 4)
        return pltpu.make_async_remote_copy(PQ.at[i], PQ.at[n_q0 + q], send_sem.at[2, i], q_sem.at[q],
                                            device_id=to(1 - r, lax.rem(j, 4)), device_id_type=MESH)

    def p_local(k, t):
        i = p_idx(k, t)
        return pltpu.make_async_remote_copy(PQ.at[i], PQ.at[i], send_sem.at[0, i], p_sem.at[i],
                                            device_id=to(r, c ^ 1), device_id_type=MESH)

    def q_local(k, s):
        q = q_idx(k, s)
        return pltpu.make_async_remote_copy(PQ.at[n_q0 + q], PQ.at[n_q0 + q], send_sem.at[2, 0], q_sem.at[q],
                                            device_id=to(1 - r, c), device_id_type=MESH)

    def each_send(k, t, act):
        kc = lax.rem(k, 4)
        i = 2 * t + r
        j = lax.rem(i, 4)
        far = i > k + 1
        own = c == kc

        @pl.when(own & far)
        def _():
            act(p_copy(k, t, 1, across(k)))
            act(p_copy(k, t, 0, c ^ 1))

        @pl.when(own & (i < LAST) & (jnp.logical_not(far) | (j // 2 == kc // 2)))
        def _():
            act(q_copy(k, t))

        @pl.when((c == across(k)) & far)
        def _():
            act(p_copy(k, t, 0, c ^ 1))

            @pl.when((i < LAST) & (j == (c ^ 1)))
            def _():
                act(q_copy(k, t))

    def near_view(k, n):
        i = p_idx(k, (k + 1) // 2)
        if n < 2:
            return PQ.at[i, :, SUB * n:SUB * (n + 1)]
        return PQ.at[i, SUB * (n - 2):SUB * (n - 1), 2 * SUB:BS]

    def near_copy(k, n):
        return pltpu.make_async_remote_copy(near_view(k, n), near_view(k, n), us_sem.at[k, n], ur_sem.at[k, n],
                                            device_id=to(r, lax.rem(k + 1, 4)), device_id_type=MESH)

    def near_local(k, n):
        return pltpu.make_async_remote_copy(near_view(k, n), near_view(k, n), us_sem.at[k, n], ur_sem.at[k, n],
                                            device_id=to(r, lax.rem(k, 4)), device_id_type=MESH)

    def recv(k, t):
        p_local(k, t).wait_recv()

    def forward(k, t):
        recv(k, t)
        each_send(k, t, lambda cp: cp.start())

    def col_index(k, s):
        return jnp.where(same, p_idx(k, 2 * s + (c - r) // 2), n_q0 + q_idx(k, s))

    def update(k, t, s):
        @pl.when(k == 0)
        def _():
            load(t, s).wait()
        prod = lax.dot_general(PQ[p_idx(k, t)], PQ[col_index(k, s)], (((1,), (1,)), ((), ())),
                               preferred_element_type=F32)
        S[t, :, blk(s)] = S[t, :, blk(s)] - prod

    def fb_copy(slot, b):
        view = FB.at[slot, b, :, SUB * b:BS]
        return pltpu.make_async_remote_copy(view, view, fs_sem.at[slot, b], fr_sem.at[slot, b],
                                            device_id=to(1 - r, c), device_id_type=MESH)

    def load(t, s):
        return pltpu.make_async_copy(a_hbm.at[t, :, blk(s)], S.at[t, :, blk(s)], ld_sem.at[t, s])

    def store(t, s):
        return pltpu.make_async_copy(S.at[t, :, blk(s)], o_hbm.at[t, :, blk(s)], st_sem.at[t, s])

    def lower(t, s):
        return 2 * t + r >= 4 * s + c

    def all_blocks(fn):
        def body(n, _):
            fn(lax.rem(n, 8), n // 8)
            return 0
        lax.fori_loop(0, 32, body, 0)

    def begin(t, s):
        @pl.when(lower(t, s))
        def _():
            load(t, s).start()

    def blank_copy(t, s):
        return pltpu.make_async_copy(S.at[0, :, 3 * BS:4 * BS], o_hbm.at[t, :, blk(s)], st_sem.at[t, s])

    def blank(t, s):
        @pl.when(jnp.logical_not(lower(t, s)))
        def _():
            blank_copy(t, s).start()

    barrier = pltpu.get_barrier_semaphore()
    all_blocks(begin)
    for step in range(1, 8):
        dr, dc = step // 4, step % 4
        pl.semaphore_signal(barrier, inc=1, device_id=to(r ^ dr, c ^ dc), device_id_type=MESH)
    S[0, :, 3 * BS:4 * BS] = jnp.zeros((BS, BS), F32)
    pl.semaphore_wait(barrier, 7)

    def bf_dot(x, y):
        return lax.dot_general(x, y, (((1,), (1,)), ((), ())), preferred_element_type=F32)

    def shrink(row, col, part):
        D[row:row + SUB, col:BS] = D[row:row + SUB, col:BS] - bf_dot(part[row:row + SUB], part[col:BS])

    def factor_diag(slot, more, late):
        def tile(b, _):
            off = pl.multiple_of(b * SUB, SUB)
            factor_tile(D, off, ub.at[b], wb, sc)
            w = wb[...]
            FB[slot, b, :, pl.ds(off, SUB)] = w

            @pl.when(b == 0)
            def _():
                late()
                rest = dot_hi(w, D[0:SUB, SUB:BS], ((1,), (0,)))
                FB[slot, 0, :, SUB:BS] = rest
                @pl.when(more)
                def _():
                    fb_copy(slot, 0).start()
                D[SUB:BS, SUB:BS] = D[SUB:BS, SUB:BS] - dot_hi(rest, rest, ((0,), (0,)))

            @pl.when(b == 1)
            def _():
                rest = dot_hi(w, D[SUB:2 * SUB, 2 * SUB:BS], ((1,), (0,)))
                FB[slot, 1, :, 2 * SUB:BS] = rest
                @pl.when(more)
                def _():
                    fb_copy(slot, 1).start()
                D[2 * SUB:BS, 2 * SUB:BS] = D[2 * SUB:BS, 2 * SUB:BS] - dot_hi(rest, rest, ((0,), (0,)))

            @pl.when(b == 2)
            def _():
                @pl.when(more)
                def _():
                    fb_copy(slot, 2).start()
            return 0
        lax.fori_loop(0, 3, tile, 0)

    def solve(k, t, s, ready, done, pieces):
        idx = p_idx(k, t)

        def tile(n):
            return pl.ds(pl.multiple_of(s * BS + SUB * n, SUB), SUB)

        def put(n, x):
            PQ[idx, :, SUB * n:SUB * (n + 1)] = x.astype(BF16)
            S[t, :, tile(n)] = x
            done(n)

        ready(0)
        x1 = dot_hi(S[t, :, tile(0)], FB[s, 0, :, 0:SUB], ((1,), (1,)))
        put(0, x1)
        rest = S[t, :, pl.ds(pl.multiple_of(s * BS + SUB, SUB), 2 * SUB)] - dot_hi(x1, FB[s, 0, :, SUB:BS], ((1,), (0,)))
        ready(1)
        x2 = dot_hi(rest[:, 0:SUB], FB[s, 1, :, SUB:2 * SUB], ((1,), (1,)))
        put(1, x2)
        last = rest[:, SUB:2 * SUB] - dot_hi(x2, FB[s, 1, :, 2 * SUB:BS], ((1,), (0,)))
        ready(2)
        rows = BS // pieces
        for h in range(pieces):
            at = slice(rows * h, rows * (h + 1))
            x3 = dot_hi(last[at], FB[s, 2, :, 2 * SUB:BS], ((1,), (1,)))
            PQ[idx, at, 2 * SUB:BS] = x3.astype(BF16)
            S[t, at, tile(2)] = x3
            done(2 + h)

    def wave(n, _):
        kd = n // MU
        sd = kd // 4
        td = kd // 2
        diag = (lax.rem(n, MU) == 0) & (c == lax.rem(kd, 4)) & (r == lax.rem(kd, 2))

        @pl.when(diag)
        def _():
            @pl.when(kd > 0)
            def _():
                @pl.when(kd == 1)
                def _():
                    load(td, sd).wait()
                D[...] = S[td, :, blk(sd)]
                idx = p_idx(kd - 1, td)
                for e in range(2):
                    near_local(kd - 1, e).wait_recv()
                    part = PQ[idx, :, SUB * e:SUB * (e + 1)]
                    for b in range(0, BS, SUB):
                        shrink(b, b, part)
                near_local(kd - 1, 2).wait_recv()
                top = PQ[idx, 0:SUB, 2 * SUB:BS]
                D[0:SUB, 0:SUB] = D[0:SUB, 0:SUB] - bf_dot(top, top)

            @pl.when(kd == 0)
            def _():
                load(td, sd).wait()
                D[...] = S[td, :, blk(sd)]

            def late():
                @pl.when(kd > 0)
                def _():
                    for e in range(3, 5):
                        near_local(kd - 1, e).wait_recv()
                    part = PQ[p_idx(kd - 1, td), :, 2 * SUB:BS]
                    shrink(0, SUB, part)
                    shrink(SUB, SUB, part)
                    shrink(2 * SUB, 2 * SUB, part)
            factor_diag(sd, kd < NB - 1, late)

        def span(v):
            par = lax.rem(v + r, 2)
            lo = (jnp.maximum(v - (NB - 1) + LAG - 1, 0) // LAG + 1 - par) // 2
            hi = ((v + MU - 2) // MU + 1 - par) // 2
            return par, lo, hi

        def pass_on(v):
            par, lo, hi = span(v)

            def one(m, _):
                k = 2 * m + par

                @pl.when(c == across(k))
                def _():
                    forward(k, (v - LAG * k - r) // 2)
                return 0
            lax.fori_loop(lo, hi, one, 0)

        @pl.when((n >= HOP) & ((lax.rem(n, MU) != 2) | (c != lax.rem(kd, 4)) | (r != lax.rem(kd + 1, 2))))
        def _():
            pass_on(n - HOP)

        near = (lax.rem(n, MU) == 1) & (c == lax.rem(kd, 4)) & (r == lax.rem(kd + 1, 2))

        @pl.when(near)
        def _():
            t = (kd + 1) // 2

            @pl.when(kd == 0)
            def _():
                load(t, sd).wait()

            @pl.when(kd > 0)
            def _():
                q_local(kd - 1, sd).wait_recv()

                @pl.when(lax.rem(kd, 2) == 1)
                def _():
                    recv(kd - 1, t)
                update(kd - 1, t, sd)

            def ready(e):
                if e == 1:
                    pass_on(n + 1 - HOP)
                fb_copy(sd, e).wait_recv()
            solve(kd, t, sd, ready, lambda e: near_copy(kd, e).start(), 3)
            each_send(kd, t, lambda cp: cp.start())
            store(t, sd).start()

        @pl.when(n >= LAG)
        def _():
            v = n - LAG
            par, lo, hi = span(v)
            hi = hi - jnp.where(near & (kd > 0), 1, 0)

            def arrive(m, _):
                k = 2 * m + par

                @pl.when((c != lax.rem(k, 4)) & (c != across(k)))
                def _():
                    recv(k, (v - LAG * k - r) // 2)
                return 0
            lax.fori_loop(lo, hi, arrive, 0)

            @pl.when(jnp.logical_not(same))
            def _():
                def arrive_q(s, _):
                    j = 4 * s + c
                    d = v - 1 - j

                    @pl.when((j < LAST) & (d >= 0) & (lax.rem(d, LAG) == 0) & (d < LAG * (j - 1)))
                    def _():
                        q_local(d // LAG, s).wait_recv()
                    return 0
                lax.fori_loop(0, 4, arrive_q, 0)

        @pl.when(lax.rem(n + c, 2) == r)
        def _():
            def task(m, _):
                s = 3 - m
                k = 4 * s + c
                i = n - LAG * k

                @pl.when((i > k + 1) & (i < NB))
                def _():
                    t = (i - r) // 2

                    @pl.when(k == 0)
                    def _():
                        load(t, s).wait()

                    @pl.when(k > 0)
                    def _():
                        update(k - 1, t, s)
                    solve(k, t, s, lambda e: None, lambda e: None, 1)
                    each_send(k, t, lambda cp: cp.start())
                    store(t, s).start()
                return 0
            lax.fori_loop(0, 4, task, 0)

        @pl.when(n >= LAG)
        def _():
            v = n - LAG
            par, lo, hi = span(v)
            hi = hi - jnp.where(near & (kd > 0), 1, 0)

            def apply(m, _):
                k = 2 * m + par
                i = v - LAG * k

                def one(s, _):
                    @pl.when(4 * s + c != k + 1)
                    def _():
                        update(k, (i - r) // 2, s)
                    return 0
                lax.fori_loop((k + 4 - c) // 4, (i + 4 - c) // 4, one, 0)
                return 0
            lax.fori_loop(lo, hi, apply, 0)

        @pl.when(diag)
        def _():
            for b in range(3):
                S[td, SUB * b:SUB * (b + 1), pl.ds(pl.multiple_of(sd * BS + SUB * b, SUB), SUB)] = ub[b].T
                for e in range(b + 1, 3):
                    S[td, SUB * e:SUB * (e + 1), pl.ds(pl.multiple_of(sd * BS + SUB * b, SUB), SUB)] = FB[sd, b, :, SUB * e:SUB * (e + 1)].T
                    S[td, SUB * b:SUB * (b + 1), pl.ds(pl.multiple_of(sd * BS + SUB * e, SUB), SUB)] = jnp.zeros((SUB, SUB), F32)
            store(td, sd).start()

        @pl.when(n == 1)
        def _():
            all_blocks(blank)
        return 0

    lax.fori_loop(0, MU * (NB - 1) + 1, wave, 0)

    def drain(k, _):
        t0 = first_t(k)
        own = c == lax.rem(k, 4)

        def one(t, _):
            each_send(k, t, lambda cp: cp.wait_send())
            return 0
        lax.fori_loop(t0, 8, one, 0)

        @pl.when(own & (k < NB - 1))
        def _():
            @pl.when(r == lax.rem(k, 2))
            def _():
                for b in range(3):
                    fb_copy(k // 4, b).wait_send()

            @pl.when(r != lax.rem(k, 2))
            def _():
                for b in range(5):
                    near_copy(k, b).wait_send()
        return 0
    lax.fori_loop(0, NB, drain, 0)
    all_blocks(lambda t, s: store(t, s).wait())


def solution(mesh):
    def local(a):
        return pl.pallas_call(
            kernel,
            out_shape=jax.ShapeDtypeStruct(a.shape, F32),
            in_specs=[pl.BlockSpec(memory_space=pl.ANY)],
            out_specs=pl.BlockSpec(memory_space=pl.ANY),
            scratch_shapes=[
                pltpu.VMEM((8, BS, 4 * BS), F32),
                pltpu.VMEM((104, BS, BS), BF16),
                pltpu.VMEM((4, 3, SUB, BS), F32),
                pltpu.VMEM((BS, BS), F32),
                pltpu.VMEM((3, SUB, SUB), F32),
                pltpu.VMEM((SUB, SUB), F32),
                pltpu.VMEM((320, SUB), F32),
                pltpu.SemaphoreType.DMA((8, 4)),
                pltpu.SemaphoreType.DMA((8, 4)),
                pltpu.SemaphoreType.DMA((3, 64)),
                pltpu.SemaphoreType.DMA((64,)),
                pltpu.SemaphoreType.DMA((40,)),
                pltpu.SemaphoreType.DMA((4, 3)),
                pltpu.SemaphoreType.DMA((4, 3)),
                pltpu.SemaphoreType.DMA((16, 5)),
                pltpu.SemaphoreType.DMA((16, 5)),
            ],
            compiler_params=pltpu.CompilerParams(collective_id=0, has_side_effects=True,
                                                 vmem_limit_bytes=67043328),
            name="cholesky",
        )(a)

    spec = P(("batch", "row"), None, "col")
    return jax.shard_map(local, mesh=mesh, in_specs=(spec,), out_specs=spec, check_vma=False)
```

```python
import functools
import jax
import jax.numpy as jnp
from jax import lax
from jax.experimental import pallas as pl
from jax.experimental.pallas import tpu as pltpu
from jax.sharding import PartitionSpec as P

F32 = jnp.float32
BF16 = jnp.bfloat16
NB = 16
BS = 384
SUB = 128
MU = 4
LAG = MU - 1
HOP = MU // 2
LAST = NB - 1
MESH = pl.DeviceIdType.MESH


def dot_hi(a, b, dims):
    return lax.dot_general(a, b, (dims, ((), ())), precision=lax.Precision.HIGHEST, preferred_element_type=F32)


def lane_splat(x, i):
    return jnp.broadcast_to(x[:, i:i + 1], (8, SUB))


def row_splat(ref, row):
    return jnp.broadcast_to(ref[row:row + 1, :], (8, SUB))


def factor_tile(d_ref, off, u_ref, w_ref, sc):
    lane = lax.broadcasted_iota(jnp.int32, (8, SUB), 1)
    sub = lax.broadcasted_iota(jnp.int32, (8, SUB), 0)
    n_oct = SUB // 8
    half = n_oct // 2
    X = [d_ref[pl.ds(pl.multiple_of(off + 8 * t, 8), 8), pl.ds(off, SUB)] for t in range(n_oct)]
    nxt = [lane_splat(X[0], i) for i in range(8)]
    for t in range(n_oct):
        j = 8 * t
        o = 160 * (t % 2)
        rows = X[t]
        for i in range(8):
            sc[o + 8 * i:o + 8 * i + 8, :] = nxt[i]
        d = {(m, i): row_splat(sc, o + 8 * i + m) for i in range(8) for m in range(i, 8)}
        sc[o + 64:o + 72, :] = rows
        sc[o + 72:o + 80, :] = jnp.where(lane < j, rows, jnp.where(lane == sub + j, 1.0, 0.0))
        inv = [None] * 8
        low = {}
        for i in range(8):
            inv[i] = lax.rsqrt(d[i, i])
            for m in range(i + 1, 8):
                low[m, i] = d[m, i] * inv[i]
            for m in range(i + 1, 8):
                for n in range(i + 1, m + 1):
                    d[m, n] = d[m, n] - low[m, i] * low[n, i]

        def column(s):
            c = []
            for i in range(8):
                x = lane_splat(X[s], j + i)
                for p in range(i):
                    x = x - low[i, p] * c[p]
                c.append(x * inv[i])
            return c

        end = (t // half + 1) * half
        if t + 1 < end:
            first = column(t + 1)
            nxt = [lane_splat(X[t + 1], j + 8 + m) for m in range(8)]
            for i in range(8):
                sc[o + 80 + 8 * i:o + 88 + 8 * i, :] = first[i]
            for i in range(8):
                for m in range(8):
                    nxt[m] = nxt[m] - first[i] * row_splat(sc, o + 80 + 8 * i + m)
        u = []
        w = []
        for i in range(8):
            x = row_splat(sc, o + 64 + i)
            y = row_splat(sc, o + 72 + i)
            for p in range(i):
                x = x - low[i, p] * u[p]
                y = y - low[i, p] * w[p]
            u.append(x * inv[i])
            w.append(y * inv[i])
        u8 = u[7]
        w8 = w[7]
        for i in range(7):
            u8 = jnp.where(sub == i, u[i], u8)
            w8 = jnp.where(sub == i, w[i], w8)
        u_ref[j:j + 8, :] = jnp.where(lane >= sub + j, u8, 0.0)
        w_ref[j:j + 8, :] = jnp.where(lane < j + 8, w8, 0.0)
        z = [jnp.where(lane < j + 8, w[i], u[i]) for i in range(8)]
        for s in range(t + 1, end):
            c = first if s == t + 1 else column(s)
            x = jnp.where((lane >= j) & (lane < j + 8), 0.0, X[s])
            for i in range(8):
                x = x - c[i] * z[i]
            X[s] = x
        if t + 1 == half:
            e = 8 * half
            top = u_ref[0:e, :]
            z = jnp.where(lax.broadcasted_iota(jnp.int32, (e, SUB), 1) < e, w_ref[0:e, :], top)
            prod = dot_hi(top[:, e:SUB], z, ((0,), (0,)))
            for s in range(half, n_oct):
                X[s] = jnp.where(lane < e, 0.0, X[s]) - prod[8 * (s - half):8 * (s - half + 1), :]
            nxt = [lane_splat(X[half], e + m) for m in range(8)]


def kernel(a_hbm, S, PQ, FB, D, ub, wb, sc, ld_sem, send_sem, p_sem, q_sem, fs_sem, fr_sem, us_sem, ur_sem):
    g = lax.axis_index("batch")
    r = lax.axis_index("row")
    c = lax.axis_index("col")
    n_q0 = 64
    same = r == lax.rem(c, 2)

    def blk(s):
        return pl.ds(pl.multiple_of(s * BS, SUB), BS)

    def p_idx(k, t):
        return 8 * k - (k // 2) * ((k + 1) // 2) + t - (k + 1) // 2

    def q_idx(k, s):
        m = k // 4
        return 4 * k - (4 * (m * (m - 1) // 2) + (k - 4 * m) * m) + s - m

    def first_t(k):
        return (k + 2 - r) // 2

    def to(row, col):
        return (g, row, col)

    def across(k):
        kc = lax.rem(k, 4)
        return jnp.where(lax.rem(kc, 2) == r, kc ^ 3, kc ^ 2)

    def p_copy(k, t, kind, col):
        i = p_idx(k, t)
        return pltpu.make_async_remote_copy(PQ.at[i], PQ.at[i], send_sem.at[kind, i], p_sem.at[i],
                                            device_id=to(r, col), device_id_type=MESH)

    def q_copy(k, t):
        i = p_idx(k, t)
        j = 2 * t + r
        q = q_idx(k, j // 4)
        return pltpu.make_async_remote_copy(PQ.at[i], PQ.at[n_q0 + q], send_sem.at[2, i], q_sem.at[q],
                                            device_id=to(1 - r, lax.rem(j, 4)), device_id_type=MESH)

    def p_local(k, t):
        i = p_idx(k, t)
        return pltpu.make_async_remote_copy(PQ.at[i], PQ.at[i], send_sem.at[0, i], p_sem.at[i],
                                            device_id=to(r, c ^ 1), device_id_type=MESH)

    def q_local(k, s):
        q = q_idx(k, s)
        return pltpu.make_async_remote_copy(PQ.at[n_q0 + q], PQ.at[n_q0 + q], send_sem.at[2, 0], q_sem.at[q],
                                            device_id=to(1 - r, c), device_id_type=MESH)

    def each_send(k, t, act):
        kc = lax.rem(k, 4)
        i = 2 * t + r
        j = lax.rem(i, 4)
        far = i > k + 1
        own = c == kc

        @pl.when(own & far)
        def _():
            act(p_copy(k, t, 1, across(k)))
            act(p_copy(k, t, 0, c ^ 1))

        @pl.when(own & (i < LAST) & (jnp.logical_not(far) | (j // 2 == kc // 2)))
        def _():
            act(q_copy(k, t))

        @pl.when((c == across(k)) & far)
        def _():
            act(p_copy(k, t, 0, c ^ 1))

            @pl.when((i < LAST) & (j == (c ^ 1)))
            def _():
                act(q_copy(k, t))

    def near_view(k, n):
        i = p_idx(k, (k + 1) // 2)
        if n < 2:
            return PQ.at[i, :, SUB * n:SUB * (n + 1)]
        return PQ.at[i, SUB * (n - 2):SUB * (n - 1), 2 * SUB:BS]

    def near_copy(k, n):
        return pltpu.make_async_remote_copy(near_view(k, n), near_view(k, n), us_sem.at[k, n], ur_sem.at[k, n],
                                            device_id=to(r, lax.rem(k + 1, 4)), device_id_type=MESH)

    def near_local(k, n):
        return pltpu.make_async_remote_copy(near_view(k, n), near_view(k, n), us_sem.at[k, n], ur_sem.at[k, n],
                                            device_id=to(r, lax.rem(k, 4)), device_id_type=MESH)

    def recv(k, t):
        p_local(k, t).wait_recv()

    def forward(k, t):
        recv(k, t)
        each_send(k, t, lambda cp: cp.start())

    def col_index(k, s):
        return jnp.where(same, p_idx(k, 2 * s + (c - r) // 2), n_q0 + q_idx(k, s))

    def update(k, t, s):
        @pl.when(k == 0)
        def _():
            load(t, s).wait()
        prod = lax.dot_general(PQ[p_idx(k, t)], PQ[col_index(k, s)], (((1,), (1,)), ((), ())),
                               preferred_element_type=F32)
        S[t, :, blk(s)] = S[t, :, blk(s)] - prod

    def fb_copy(slot, b):
        view = FB.at[slot, b, :, SUB * b:BS]
        return pltpu.make_async_remote_copy(view, view, fs_sem.at[slot, b], fr_sem.at[slot, b],
                                            device_id=to(1 - r, c), device_id_type=MESH)

    def load(t, s):
        return pltpu.make_async_copy(a_hbm.at[t, :, blk(s)], S.at[t, :, blk(s)], ld_sem.at[t, s])

    def lower(t, s):
        return 2 * t + r >= 4 * s + c

    def all_blocks(fn):
        def body(n, _):
            fn(lax.rem(n, 8), n // 8)
            return 0
        lax.fori_loop(0, 32, body, 0)

    def begin(t, s):
        @pl.when(lower(t, s))
        def _():
            load(t, s).start()

    def blank(t, s):
        @pl.when(jnp.logical_not(lower(t, s)))
        def _():
            S[t, :, blk(s)] = jnp.zeros((BS, BS), F32)

    barrier = pltpu.get_barrier_semaphore()
    all_blocks(begin)
    for step in range(1, 8):
        dr, dc = step // 4, step % 4
        pl.semaphore_signal(barrier, inc=1, device_id=to(r ^ dr, c ^ dc), device_id_type=MESH)
    pl.semaphore_wait(barrier, 7)

    def bf_dot(x, y):
        return lax.dot_general(x, y, (((1,), (1,)), ((), ())), preferred_element_type=F32)

    def shrink(row, col, part):
        D[row:row + SUB, col:BS] = D[row:row + SUB, col:BS] - bf_dot(part[row:row + SUB], part[col:BS])

    def factor_diag(slot, more, late):
        def tile(b, _):
            off = pl.multiple_of(b * SUB, SUB)
            factor_tile(D, off, ub.at[b], wb, sc)
            w = wb[...]
            FB[slot, b, :, pl.ds(off, SUB)] = w

            @pl.when(b == 0)
            def _():
                late()
                rest = dot_hi(w, D[0:SUB, SUB:BS], ((1,), (0,)))
                FB[slot, 0, :, SUB:BS] = rest
                @pl.when(more)
                def _():
                    fb_copy(slot, 0).start()
                D[SUB:BS, SUB:BS] = D[SUB:BS, SUB:BS] - dot_hi(rest, rest, ((0,), (0,)))

            @pl.when(b == 1)
            def _():
                rest = dot_hi(w, D[SUB:2 * SUB, 2 * SUB:BS], ((1,), (0,)))
                FB[slot, 1, :, 2 * SUB:BS] = rest
                @pl.when(more)
                def _():
                    fb_copy(slot, 1).start()
                D[2 * SUB:BS, 2 * SUB:BS] = D[2 * SUB:BS, 2 * SUB:BS] - dot_hi(rest, rest, ((0,), (0,)))

            @pl.when(b == 2)
            def _():
                @pl.when(more)
                def _():
                    fb_copy(slot, 2).start()
            return 0
        lax.fori_loop(0, 3, tile, 0)

    def solve(k, t, s, ready, done, pieces):
        idx = p_idx(k, t)

        def tile(n):
            return pl.ds(pl.multiple_of(s * BS + SUB * n, SUB), SUB)

        def put(n, x):
            PQ[idx, :, SUB * n:SUB * (n + 1)] = x.astype(BF16)
            S[t, :, tile(n)] = x
            done(n)

        ready(0)
        x1 = dot_hi(S[t, :, tile(0)], FB[s, 0, :, 0:SUB], ((1,), (1,)))
        put(0, x1)
        rest = S[t, :, pl.ds(pl.multiple_of(s * BS + SUB, SUB), 2 * SUB)] - dot_hi(x1, FB[s, 0, :, SUB:BS], ((1,), (0,)))
        ready(1)
        x2 = dot_hi(rest[:, 0:SUB], FB[s, 1, :, SUB:2 * SUB], ((1,), (1,)))
        put(1, x2)
        last = rest[:, SUB:2 * SUB] - dot_hi(x2, FB[s, 1, :, 2 * SUB:BS], ((1,), (0,)))
        ready(2)
        rows = BS // pieces
        for h in range(pieces):
            at = slice(rows * h, rows * (h + 1))
            x3 = dot_hi(last[at], FB[s, 2, :, 2 * SUB:BS], ((1,), (1,)))
            PQ[idx, at, 2 * SUB:BS] = x3.astype(BF16)
            S[t, at, tile(2)] = x3
            done(2 + h)

    def wave(n, _):
        kd = n // MU
        sd = kd // 4
        td = kd // 2
        diag = (lax.rem(n, MU) == 0) & (c == lax.rem(kd, 4)) & (r == lax.rem(kd, 2))

        @pl.when(diag)
        def _():
            @pl.when(kd > 0)
            def _():
                @pl.when(kd == 1)
                def _():
                    load(td, sd).wait()
                D[...] = S[td, :, blk(sd)]
                idx = p_idx(kd - 1, td)
                for e in range(2):
                    near_local(kd - 1, e).wait_recv()
                    part = PQ[idx, :, SUB * e:SUB * (e + 1)]
                    for b in range(0, BS, SUB):
                        shrink(b, b, part)
                near_local(kd - 1, 2).wait_recv()
                top = PQ[idx, 0:SUB, 2 * SUB:BS]
                D[0:SUB, 0:SUB] = D[0:SUB, 0:SUB] - bf_dot(top, top)

            @pl.when(kd == 0)
            def _():
                load(td, sd).wait()
                D[...] = S[td, :, blk(sd)]

            def late():
                @pl.when(kd > 0)
                def _():
                    for e in range(3, 5):
                        near_local(kd - 1, e).wait_recv()
                    part = PQ[p_idx(kd - 1, td), :, 2 * SUB:BS]
                    shrink(0, SUB, part)
                    shrink(SUB, SUB, part)
                    shrink(2 * SUB, 2 * SUB, part)
            factor_diag(sd, kd < NB - 1, late)

        def span(v):
            par = lax.rem(v + r, 2)
            lo = (jnp.maximum(v - (NB - 1) + LAG - 1, 0) // LAG + 1 - par) // 2
            hi = ((v + MU - 2) // MU + 1 - par) // 2
            return par, lo, hi

        def pass_on(v):
            par, lo, hi = span(v)

            def one(m, _):
                k = 2 * m + par

                @pl.when(c == across(k))
                def _():
                    forward(k, (v - LAG * k - r) // 2)
                return 0
            lax.fori_loop(lo, hi, one, 0)

        @pl.when((n >= HOP) & ((lax.rem(n, MU) != 2) | (c != lax.rem(kd, 4)) | (r != lax.rem(kd + 1, 2))))
        def _():
            pass_on(n - HOP)

        near = (lax.rem(n, MU) == 1) & (c == lax.rem(kd, 4)) & (r == lax.rem(kd + 1, 2))

        @pl.when(near)
        def _():
            t = (kd + 1) // 2

            @pl.when(kd == 0)
            def _():
                load(t, sd).wait()

            @pl.when(kd > 0)
            def _():
                q_local(kd - 1, sd).wait_recv()

                @pl.when(lax.rem(kd, 2) == 1)
                def _():
                    recv(kd - 1, t)
                update(kd - 1, t, sd)

            def ready(e):
                if e == 1:
                    pass_on(n + 1 - HOP)
                fb_copy(sd, e).wait_recv()
            solve(kd, t, sd, ready, lambda e: near_copy(kd, e).start(), 3)
            each_send(kd, t, lambda cp: cp.start())

        @pl.when(n >= LAG)
        def _():
            v = n - LAG
            par, lo, hi = span(v)
            hi = hi - jnp.where(near & (kd > 0), 1, 0)

            def arrive(m, _):
                k = 2 * m + par

                @pl.when((c != lax.rem(k, 4)) & (c != across(k)))
                def _():
                    recv(k, (v - LAG * k - r) // 2)
                return 0
            lax.fori_loop(lo, hi, arrive, 0)

            @pl.when(jnp.logical_not(same))
            def _():
                def arrive_q(s, _):
                    j = 4 * s + c
                    d = v - 1 - j

                    @pl.when((j < LAST) & (d >= 0) & (lax.rem(d, LAG) == 0) & (d < LAG * (j - 1)))
                    def _():
                        q_local(d // LAG, s).wait_recv()
                    return 0
                lax.fori_loop(0, 4, arrive_q, 0)

        @pl.when(lax.rem(n + c, 2) == r)
        def _():
            def task(m, _):
                s = 3 - m
                k = 4 * s + c
                i = n - LAG * k

                @pl.when((i > k + 1) & (i < NB))
                def _():
                    t = (i - r) // 2

                    @pl.when(k == 0)
                    def _():
                        load(t, s).wait()

                    @pl.when(k > 0)
                    def _():
                        update(k - 1, t, s)
                    solve(k, t, s, lambda e: None, lambda e: None, 1)
                    each_send(k, t, lambda cp: cp.start())
                return 0
            lax.fori_loop(0, 4, task, 0)

        @pl.when(n >= LAG)
        def _():
            v = n - LAG
            par, lo, hi = span(v)
            hi = hi - jnp.where(near & (kd > 0), 1, 0)

            def apply(m, _):
                k = 2 * m + par
                i = v - LAG * k

                def one(s, _):
                    @pl.when(4 * s + c != k + 1)
                    def _():
                        update(k, (i - r) // 2, s)
                    return 0
                lax.fori_loop((k + 4 - c) // 4, (i + 4 - c) // 4, one, 0)
                return 0
            lax.fori_loop(lo, hi, apply, 0)

        @pl.when(diag)
        def _():
            for b in range(3):
                S[td, SUB * b:SUB * (b + 1), pl.ds(pl.multiple_of(sd * BS + SUB * b, SUB), SUB)] = ub[b].T
                for e in range(b + 1, 3):
                    S[td, SUB * e:SUB * (e + 1), pl.ds(pl.multiple_of(sd * BS + SUB * b, SUB), SUB)] = FB[sd, b, :, SUB * e:SUB * (e + 1)].T
                    S[td, SUB * b:SUB * (b + 1), pl.ds(pl.multiple_of(sd * BS + SUB * e, SUB), SUB)] = jnp.zeros((SUB, SUB), F32)

        @pl.when(n == 2)
        def _():
            all_blocks(blank)
        return 0

    lax.fori_loop(0, MU * (NB - 1) + 1, wave, 0)

    def drain(k, _):
        t0 = first_t(k)
        own = c == lax.rem(k, 4)

        def one(t, _):
            each_send(k, t, lambda cp: cp.wait_send())
            return 0
        lax.fori_loop(t0, 8, one, 0)

        @pl.when(own & (k < NB - 1))
        def _():
            @pl.when(r == lax.rem(k, 2))
            def _():
                for b in range(3):
                    fb_copy(k // 4, b).wait_send()

            @pl.when(r != lax.rem(k, 2))
            def _():
                for b in range(5):
                    near_copy(k, b).wait_send()
        return 0
    lax.fori_loop(0, NB, drain, 0)


def solution(mesh):
    def local(a):
        return pl.pallas_call(
            kernel,
            out_shape=pltpu.VMEM(a.shape, F32),
            in_specs=[pl.BlockSpec(memory_space=pl.ANY)],
            out_specs=pl.BlockSpec(memory_space=pltpu.VMEM),
            scratch_shapes=[
                pltpu.VMEM((104, BS, BS), BF16),
                pltpu.VMEM((4, 3, SUB, BS), F32),
                pltpu.VMEM((BS, BS), F32),
                pltpu.VMEM((3, SUB, SUB), F32),
                pltpu.VMEM((SUB, SUB), F32),
                pltpu.VMEM((320, SUB), F32),
                pltpu.SemaphoreType.DMA((8, 4)),
                pltpu.SemaphoreType.DMA((3, 64)),
                pltpu.SemaphoreType.DMA((64,)),
                pltpu.SemaphoreType.DMA((40,)),
                pltpu.SemaphoreType.DMA((4, 3)),
                pltpu.SemaphoreType.DMA((4, 3)),
                pltpu.SemaphoreType.DMA((16, 5)),
                pltpu.SemaphoreType.DMA((16, 5)),
            ],
            compiler_params=pltpu.CompilerParams(collective_id=0, has_side_effects=True,
                                                 vmem_limit_bytes=44 * 2 ** 20),
            name="cholesky",
        )(a)

    spec = P(("batch", "row"), None, "col")
    return jax.shard_map(local, mesh=mesh, in_specs=(spec,), out_specs=spec, check_vma=False)
```

```python
import functools
import jax
import jax.numpy as jnp
from jax import lax
from jax.experimental import pallas as pl
from jax.experimental.pallas import tpu as pltpu
from jax.sharding import PartitionSpec as P

F32 = jnp.float32
BF16 = jnp.bfloat16
NB = 16
BS = 384
SUB = 128
MU = 4
LAG = MU - 1
HOP = MU // 2
LAST = NB - 1
MESH = pl.DeviceIdType.MESH


def dot_hi(a, b, dims):
    return lax.dot_general(a, b, (dims, ((), ())), precision=lax.Precision.HIGHEST, preferred_element_type=F32)


def lane_splat(x, i):
    return jnp.broadcast_to(x[:, i:i + 1], (8, SUB))


def row_splat(ref, row):
    return jnp.broadcast_to(ref[row:row + 1, :], (8, SUB))


def factor_tile(d_ref, off, u_ref, w_ref, sc, mid):
    lane = lax.broadcasted_iota(jnp.int32, (8, SUB), 1)
    sub = lax.broadcasted_iota(jnp.int32, (8, SUB), 0)
    n_oct = SUB // 8
    half = n_oct // 2
    X = [d_ref[pl.ds(pl.multiple_of(off + 8 * t, 8), 8), pl.ds(off, SUB)] for t in range(n_oct)]
    nxt = [lane_splat(X[0], i) for i in range(8)]
    for t in range(n_oct):
        j = 8 * t
        o = 160 * (t % 2)
        rows = X[t]
        for i in range(8):
            sc[o + 8 * i:o + 8 * i + 8, :] = nxt[i]
        d = {(m, i): row_splat(sc, o + 8 * i + m) for i in range(8) for m in range(i, 8)}
        sc[o + 64:o + 72, :] = jnp.where((lane >= j) & (lane < j + 8), jnp.where(lane == sub + j, 1.0, 0.0), rows)
        inv = [None] * 8
        low = {}
        for i in range(8):
            inv[i] = lax.rsqrt(d[i, i])
            for m in range(i + 1, 8):
                low[m, i] = d[m, i] * inv[i]
            for m in range(i + 1, 8):
                for n in range(i + 1, m + 1):
                    d[m, n] = d[m, n] - low[m, i] * low[n, i]

        def column(s):
            c = []
            for i in range(8):
                x = lane_splat(X[s], j + i)
                for p in range(i):
                    x = x - low[i, p] * c[p]
                c.append(x * inv[i])
            return c

        end = (t // half + 1) * half
        if t + 1 < end:
            first = column(t + 1)
            nxt = [lane_splat(X[t + 1], j + 8 + m) for m in range(8)]
            for i in range(8):
                sc[o + 80 + 8 * i:o + 88 + 8 * i, :] = first[i]
            for i in range(8):
                for m in range(8):
                    nxt[m] = nxt[m] - first[i] * row_splat(sc, o + 80 + 8 * i + m)
        z = []
        for i in range(8):
            x = row_splat(sc, o + 64 + i)
            for p in range(i):
                x = x - low[i, p] * z[p]
            z.append(x * inv[i])
        z8 = z[7]
        for i in range(7):
            z8 = jnp.where(sub == i, z[i], z8)
        corner = jnp.zeros((8, SUB), F32)
        for m in range(8):
            x = d[m, m] * inv[m]
            for i in range(m):
                x = jnp.where(sub == i, low[m, i], x)
            corner = jnp.where(lane == j + m, x, corner)
        u_ref[j:j + 8, :] = jnp.where(lane >= j + 8, z8, jnp.where(lane >= sub + j, corner, 0.0))
        w_ref[j:j + 8, :] = jnp.where(lane < j + 8, z8, 0.0)
        for s in range(t + 1, end):
            c = first if s == t + 1 else column(s)
            x = jnp.where((lane >= j) & (lane < j + 8), 0.0, X[s])
            for i in range(8):
                x = x - c[i] * z[i]
            X[s] = x
        if t + 1 == half:
            e = 8 * half
            mid()
            top = u_ref[0:e, :]
            z = jnp.where(lax.broadcasted_iota(jnp.int32, (e, SUB), 1) < e, w_ref[0:e, :], top)
            prod = dot_hi(top[:, e:SUB], z, ((0,), (0,)))
            for s in range(half, n_oct):
                X[s] = jnp.where(lane < e, 0.0, X[s]) - prod[8 * (s - half):8 * (s - half + 1), :]
            nxt = [lane_splat(X[half], e + m) for m in range(8)]


def kernel(a_hbm, S, PQ, FB, D, ub, wb, sc, ld_sem, send_sem, p_sem, q_sem, fs_sem, fr_sem, us_sem, ur_sem):
    g = lax.axis_index("batch")
    r = lax.axis_index("row")
    c = lax.axis_index("col")
    n_q0 = 64
    same = r == lax.rem(c, 2)

    def blk(s):
        return pl.ds(pl.multiple_of(s * BS, SUB), BS)

    def p_idx(k, t):
        return 8 * k - (k // 2) * ((k + 1) // 2) + t - (k + 1) // 2

    def q_idx(k, s):
        m = k // 4
        return 4 * k - (4 * (m * (m - 1) // 2) + (k - 4 * m) * m) + s - m

    def first_t(k):
        return (k + 2 - r) // 2

    def to(row, col):
        return (g, row, col)

    def across(k):
        kc = lax.rem(k, 4)
        return jnp.where(lax.rem(kc, 2) == r, kc ^ 3, kc ^ 2)

    def p_copy(k, t, kind, col):
        i = p_idx(k, t)
        return pltpu.make_async_remote_copy(PQ.at[i], PQ.at[i], send_sem.at[kind, i], p_sem.at[i],
                                            device_id=to(r, col), device_id_type=MESH)

    def q_copy(k, t):
        i = p_idx(k, t)
        j = 2 * t + r
        q = q_idx(k, j // 4)
        return pltpu.make_async_remote_copy(PQ.at[i], PQ.at[n_q0 + q], send_sem.at[2, i], q_sem.at[q],
                                            device_id=to(1 - r, lax.rem(j, 4)), device_id_type=MESH)

    def p_local(k, t):
        i = p_idx(k, t)
        return pltpu.make_async_remote_copy(PQ.at[i], PQ.at[i], send_sem.at[0, i], p_sem.at[i],
                                            device_id=to(r, c ^ 1), device_id_type=MESH)

    def q_local(k, s):
        q = q_idx(k, s)
        return pltpu.make_async_remote_copy(PQ.at[n_q0 + q], PQ.at[n_q0 + q], send_sem.at[2, 0], q_sem.at[q],
                                            device_id=to(1 - r, c), device_id_type=MESH)

    def each_send(k, t, act):
        kc = lax.rem(k, 4)
        i = 2 * t + r
        j = lax.rem(i, 4)
        far = i > k + 1
        own = c == kc

        @pl.when(own & far)
        def _():
            act(p_copy(k, t, 1, across(k)))
            act(p_copy(k, t, 0, c ^ 1))

        @pl.when(own & (i < LAST) & (jnp.logical_not(far) | (j // 2 == kc // 2)))
        def _():
            act(q_copy(k, t))

        @pl.when((c == across(k)) & far)
        def _():
            act(p_copy(k, t, 0, c ^ 1))

            @pl.when((i < LAST) & (j == (c ^ 1)))
            def _():
                act(q_copy(k, t))

    def near_view(k, n):
        i = p_idx(k, (k + 1) // 2)
        if n < 2:
            return PQ.at[i, :, SUB * n:SUB * (n + 1)]
        return PQ.at[i, SUB * (n - 2):SUB * (n - 1), 2 * SUB:BS]

    def near_copy(k, n):
        return pltpu.make_async_remote_copy(near_view(k, n), near_view(k, n), us_sem.at[k, n], ur_sem.at[k, n],
                                            device_id=to(r, lax.rem(k + 1, 4)), device_id_type=MESH)

    def near_local(k, n):
        return pltpu.make_async_remote_copy(near_view(k, n), near_view(k, n), us_sem.at[k, n], ur_sem.at[k, n],
                                            device_id=to(r, lax.rem(k, 4)), device_id_type=MESH)

    def recv(k, t):
        p_local(k, t).wait_recv()

    def forward(k, t):
        recv(k, t)
        each_send(k, t, lambda cp: cp.start())

    def col_index(k, s):
        return jnp.where(same, p_idx(k, 2 * s + (c - r) // 2), n_q0 + q_idx(k, s))

    def update(k, t, s):
        @pl.when(k == 0)
        def _():
            load(t, s).wait()
        prod = lax.dot_general(PQ[p_idx(k, t)], PQ[col_index(k, s)], (((1,), (1,)), ((), ())),
                               preferred_element_type=F32)
        S[t, :, blk(s)] = S[t, :, blk(s)] - prod

    def fb_copy(slot, b):
        if b < 2:
            view = FB.at[slot, b, :, SUB * b:BS]
        else:
            view = FB.at[slot, 2, (b - 2) * SUB // 2:(b - 1) * SUB // 2, 2 * SUB:BS]
        return pltpu.make_async_remote_copy(view, view, fs_sem.at[slot, b], fr_sem.at[slot, b],
                                            device_id=to(1 - r, c), device_id_type=MESH)

    def load(t, s):
        return pltpu.make_async_copy(a_hbm.at[t, :, blk(s)], S.at[t, :, blk(s)], ld_sem.at[t, s])

    def lower(t, s):
        return 2 * t + r >= 4 * s + c

    def all_blocks(fn):
        def body(n, _):
            fn(lax.rem(n, 8), n // 8)
            return 0
        lax.fori_loop(0, 32, body, 0)

    def begin(t, s):
        @pl.when(lower(t, s))
        def _():
            load(t, s).start()

    def blank(t, s):
        @pl.when(jnp.logical_not(lower(t, s)))
        def _():
            S[t, :, blk(s)] = jnp.zeros((BS, BS), F32)

    barrier = pltpu.get_barrier_semaphore()
    all_blocks(begin)
    for step in range(1, 8):
        dr, dc = step // 4, step % 4
        pl.semaphore_signal(barrier, inc=1, device_id=to(r ^ dr, c ^ dc), device_id_type=MESH)
    pl.semaphore_wait(barrier, 7)

    def bf_dot(x, y):
        return lax.dot_general(x, y, (((1,), (1,)), ((), ())), preferred_element_type=F32)

    def shrink(row, col, part):
        D[row:row + SUB, col:BS] = D[row:row + SUB, col:BS] - bf_dot(part[row:row + SUB], part[col:BS])

    def factor_diag(slot, more, late):
        def tile(b, _):
            off = pl.multiple_of(b * SUB, SUB)
            def mid():
                @pl.when((b == 2) & more)
                def _():
                    FB[slot, 2, 0:SUB // 2, 2 * SUB:BS] = wb[0:SUB // 2, :]
                    fb_copy(slot, 2).start()

            factor_tile(D, off, ub.at[b], wb, sc, mid)
            w = wb[...]

            @pl.when(b < 2)
            def _():
                FB[slot, b, :, pl.ds(off, SUB)] = w

            @pl.when(b == 0)
            def _():
                late()
                rest = dot_hi(w, D[0:SUB, SUB:BS], ((1,), (0,)))
                FB[slot, 0, :, SUB:BS] = rest
                @pl.when(more)
                def _():
                    fb_copy(slot, 0).start()
                D[SUB:BS, SUB:BS] = D[SUB:BS, SUB:BS] - dot_hi(rest, rest, ((0,), (0,)))

            @pl.when(b == 1)
            def _():
                rest = dot_hi(w, D[SUB:2 * SUB, 2 * SUB:BS], ((1,), (0,)))
                FB[slot, 1, :, 2 * SUB:BS] = rest
                @pl.when(more)
                def _():
                    fb_copy(slot, 1).start()
                D[2 * SUB:BS, 2 * SUB:BS] = D[2 * SUB:BS, 2 * SUB:BS] - dot_hi(rest, rest, ((0,), (0,)))

            @pl.when(b == 2)
            def _():
                @pl.when(more)
                def _():
                    FB[slot, 2, SUB // 2:SUB, 2 * SUB:BS] = w[SUB // 2:SUB, :]
                    fb_copy(slot, 3).start()
            return 0
        lax.fori_loop(0, 3, tile, 0)

    def solve(k, t, s, ready, done, pieces):
        idx = p_idx(k, t)

        def tile(n):
            return pl.ds(pl.multiple_of(s * BS + SUB * n, SUB), SUB)

        def put(n, x):
            PQ[idx, :, SUB * n:SUB * (n + 1)] = x.astype(BF16)
            S[t, :, tile(n)] = x
            done(n)

        ready(0)
        x1 = dot_hi(S[t, :, tile(0)], FB[s, 0, :, 0:SUB], ((1,), (1,)))
        put(0, x1)
        rest = S[t, :, pl.ds(pl.multiple_of(s * BS + SUB, SUB), 2 * SUB)] - dot_hi(x1, FB[s, 0, :, SUB:BS], ((1,), (0,)))
        ready(1)
        x2 = dot_hi(rest[:, 0:SUB], FB[s, 1, :, SUB:2 * SUB], ((1,), (1,)))
        put(1, x2)
        last = rest[:, SUB:2 * SUB] - dot_hi(x2, FB[s, 1, :, 2 * SUB:BS], ((1,), (0,)))
        ready(2)
        rows = BS // pieces
        for h in range(pieces):
            at = slice(rows * h, rows * (h + 1))
            x3 = dot_hi(last[at], FB[s, 2, :, 2 * SUB:BS], ((1,), (1,)))
            PQ[idx, at, 2 * SUB:BS] = x3.astype(BF16)
            S[t, at, tile(2)] = x3
            done(2 + h)

    def wave(n, _):
        kd = n // MU
        sd = kd // 4
        td = kd // 2
        diag = (lax.rem(n, MU) == 0) & (c == lax.rem(kd, 4)) & (r == lax.rem(kd, 2))

        @pl.when(diag)
        def _():
            @pl.when(kd > 0)
            def _():
                @pl.when(kd == 1)
                def _():
                    load(td, sd).wait()
                D[...] = S[td, :, blk(sd)]
                idx = p_idx(kd - 1, td)
                for e in range(2):
                    near_local(kd - 1, e).wait_recv()
                    part = PQ[idx, :, SUB * e:SUB * (e + 1)]
                    for b in range(0, BS, SUB):
                        shrink(b, b, part)
                near_local(kd - 1, 2).wait_recv()
                top = PQ[idx, 0:SUB, 2 * SUB:BS]
                D[0:SUB, 0:SUB] = D[0:SUB, 0:SUB] - bf_dot(top, top)

            @pl.when(kd == 0)
            def _():
                load(td, sd).wait()
                D[...] = S[td, :, blk(sd)]

            def late():
                @pl.when(kd > 0)
                def _():
                    for e in range(3, 5):
                        near_local(kd - 1, e).wait_recv()
                    part = PQ[p_idx(kd - 1, td), :, 2 * SUB:BS]
                    shrink(0, SUB, part)
                    shrink(SUB, SUB, part)
                    shrink(2 * SUB, 2 * SUB, part)
            factor_diag(sd, kd < NB - 1, late)

        def span(v):
            par = lax.rem(v + r, 2)
            lo = (jnp.maximum(v - (NB - 1) + LAG - 1, 0) // LAG + 1 - par) // 2
            hi = ((v + MU - 2) // MU + 1 - par) // 2
            return par, lo, hi

        def pass_on(v):
            par, lo, hi = span(v)

            def one(m, _):
                k = 2 * m + par

                @pl.when(c == across(k))
                def _():
                    forward(k, (v - LAG * k - r) // 2)
                return 0
            lax.fori_loop(lo, hi, one, 0)

        @pl.when((n >= HOP) & ((lax.rem(n, MU) != 2) | (c != lax.rem(kd, 4)) | (r != lax.rem(kd + 1, 2))))
        def _():
            pass_on(n - HOP)

        near = (lax.rem(n, MU) == 1) & (c == lax.rem(kd, 4)) & (r == lax.rem(kd + 1, 2))

        @pl.when(near)
        def _():
            t = (kd + 1) // 2

            @pl.when(kd == 0)
            def _():
                load(t, sd).wait()

            @pl.when(kd > 0)
            def _():
                q_local(kd - 1, sd).wait_recv()

                @pl.when(lax.rem(kd, 2) == 1)
                def _():
                    recv(kd - 1, t)
                update(kd - 1, t, sd)

            def ready(e):
                if e == 1:
                    pass_on(n + 1 - HOP)
                fb_copy(sd, e).wait_recv()
                if e == 2:
                    fb_copy(sd, 3).wait_recv()
            solve(kd, t, sd, ready, lambda e: near_copy(kd, e).start(), 3)
            each_send(kd, t, lambda cp: cp.start())

        @pl.when(n >= LAG)
        def _():
            v = n - LAG
            par, lo, hi = span(v)
            hi = hi - jnp.where(near & (kd > 0), 1, 0)

            def arrive(m, _):
                k = 2 * m + par

                @pl.when((c != lax.rem(k, 4)) & (c != across(k)))
                def _():
                    recv(k, (v - LAG * k - r) // 2)
                return 0
            lax.fori_loop(lo, hi, arrive, 0)

            @pl.when(jnp.logical_not(same))
            def _():
                def arrive_q(s, _):
                    j = 4 * s + c
                    d = v - 1 - j

                    @pl.when((j < LAST) & (d >= 0) & (lax.rem(d, LAG) == 0) & (d < LAG * (j - 1)))
                    def _():
                        q_local(d // LAG, s).wait_recv()
                    return 0
                lax.fori_loop(0, 4, arrive_q, 0)

        @pl.when(lax.rem(n + c, 2) == r)
        def _():
            def task(m, _):
                s = 3 - m
                k = 4 * s + c
                i = n - LAG * k

                @pl.when((i > k + 1) & (i < NB))
                def _():
                    t = (i - r) // 2

                    @pl.when(k == 0)
                    def _():
                        load(t, s).wait()

                    @pl.when(k > 0)
                    def _():
                        update(k - 1, t, s)
                    solve(k, t, s, lambda e: None, lambda e: None, 1)
                    each_send(k, t, lambda cp: cp.start())
                return 0
            lax.fori_loop(0, 4, task, 0)

        @pl.when(n >= LAG)
        def _():
            v = n - LAG
            par, lo, hi = span(v)
            hi = hi - jnp.where(near & (kd > 0), 1, 0)

            def apply(m, _):
                k = 2 * m + par
                i = v - LAG * k

                def one(s, _):
                    @pl.when(4 * s + c != k + 1)
                    def _():
                        update(k, (i - r) // 2, s)
                    return 0
                lax.fori_loop((k + 4 - c) // 4, (i + 4 - c) // 4, one, 0)
                return 0
            lax.fori_loop(lo, hi, apply, 0)

        @pl.when(diag)
        def _():
            for b in range(3):
                S[td, SUB * b:SUB * (b + 1), pl.ds(pl.multiple_of(sd * BS + SUB * b, SUB), SUB)] = ub[b].T
                for e in range(b + 1, 3):
                    S[td, SUB * e:SUB * (e + 1), pl.ds(pl.multiple_of(sd * BS + SUB * b, SUB), SUB)] = FB[sd, b, :, SUB * e:SUB * (e + 1)].T
                    S[td, SUB * b:SUB * (b + 1), pl.ds(pl.multiple_of(sd * BS + SUB * e, SUB), SUB)] = jnp.zeros((SUB, SUB), F32)

        @pl.when(n == 2)
        def _():
            all_blocks(blank)
        return 0

    lax.fori_loop(0, MU * (NB - 1) + 1, wave, 0)

    def drain(k, _):
        t0 = first_t(k)
        own = c == lax.rem(k, 4)

        def one(t, _):
            each_send(k, t, lambda cp: cp.wait_send())
            return 0
        lax.fori_loop(t0, 8, one, 0)

        @pl.when(own & (k < NB - 1))
        def _():
            @pl.when(r == lax.rem(k, 2))
            def _():
                for b in range(4):
                    fb_copy(k // 4, b).wait_send()

            @pl.when(r != lax.rem(k, 2))
            def _():
                for b in range(5):
                    near_copy(k, b).wait_send()
        return 0
    lax.fori_loop(0, NB, drain, 0)


def solution(mesh):
    def local(a):
        return pl.pallas_call(
            kernel,
            out_shape=pltpu.VMEM(a.shape, F32),
            in_specs=[pl.BlockSpec(memory_space=pl.ANY)],
            out_specs=pl.BlockSpec(memory_space=pltpu.VMEM),
            scratch_shapes=[
                pltpu.VMEM((104, BS, BS), BF16),
                pltpu.VMEM((4, 3, SUB, BS), F32),
                pltpu.VMEM((BS, BS), F32),
                pltpu.VMEM((3, SUB, SUB), F32),
                pltpu.VMEM((SUB, SUB), F32),
                pltpu.VMEM((320, SUB), F32),
                pltpu.SemaphoreType.DMA((8, 4)),
                pltpu.SemaphoreType.DMA((3, 64)),
                pltpu.SemaphoreType.DMA((64,)),
                pltpu.SemaphoreType.DMA((40,)),
                pltpu.SemaphoreType.DMA((4, 4)),
                pltpu.SemaphoreType.DMA((4, 4)),
                pltpu.SemaphoreType.DMA((16, 5)),
                pltpu.SemaphoreType.DMA((16, 5)),
            ],
            compiler_params=pltpu.CompilerParams(collective_id=0, has_side_effects=True,
                                                 vmem_limit_bytes=44 * 2 ** 20),
            name="cholesky",
        )(a)

    spec = P(("batch", "row"), None, "col")
    return jax.shard_map(local, mesh=mesh, in_specs=(spec,), out_specs=spec, check_vma=False)
```

```python
import functools
import jax
import jax.numpy as jnp
from jax import lax
from jax.experimental import pallas as pl
from jax.experimental.pallas import tpu as pltpu
from jax.sharding import PartitionSpec as P

F32 = jnp.float32
BF16 = jnp.bfloat16
NB = 16
BS = 384
SUB = 128
MU = 4
LAG = MU - 1
HOP = MU // 2
LAST = NB - 1
MESH = pl.DeviceIdType.MESH


def dot_hi(a, b, dims):
    return lax.dot_general(a, b, (dims, ((), ())), precision=lax.Precision.HIGHEST, preferred_element_type=F32)


def lane_splat(x, i):
    return jnp.broadcast_to(x[:, i:i + 1], (8, SUB))


def row_splat(ref, row):
    return jnp.broadcast_to(ref[row:row + 1, :], (8, SUB))


def factor_tile(d_ref, off, u_ref, w_ref, sc, mid):
    lane = lax.broadcasted_iota(jnp.int32, (8, SUB), 1)
    sub = lax.broadcasted_iota(jnp.int32, (8, SUB), 0)
    n_oct = SUB // 8
    half = n_oct // 2
    X = [d_ref[pl.ds(pl.multiple_of(off + 8 * t, 8), 8), pl.ds(off, SUB)] for t in range(n_oct)]
    nxt = [lane_splat(X[0], i) for i in range(8)]
    for t in range(n_oct):
        j = 8 * t
        o = 160 * (t % 2)
        rows = X[t]
        for i in range(8):
            sc[o + 8 * i:o + 8 * i + 8, :] = nxt[i]
        d = {(m, i): row_splat(sc, o + 8 * i + m) for i in range(8) for m in range(i, 8)}
        sc[o + 64:o + 72, :] = jnp.where((lane >= j) & (lane < j + 8), jnp.where(lane == sub + j, 1.0, 0.0), rows)
        inv = [None] * 8
        low = {}
        for i in range(8):
            inv[i] = lax.rsqrt(d[i, i])
            for m in range(i + 1, 8):
                low[m, i] = d[m, i] * inv[i]
            for m in range(i + 1, 8):
                for n in range(i + 1, m + 1):
                    d[m, n] = d[m, n] - low[m, i] * low[n, i]

        def column(s):
            c = []
            for i in range(8):
                x = lane_splat(X[s], j + i)
                for p in range(i):
                    x = x - low[i, p] * c[p]
                c.append(x * inv[i])
            return c

        end = (t // half + 1) * half
        if t + 1 < end:
            first = column(t + 1)
            nxt = [lane_splat(X[t + 1], j + 8 + m) for m in range(8)]
            for i in range(8):
                sc[o + 80 + 8 * i:o + 88 + 8 * i, :] = first[i]
            for i in range(8):
                for m in range(8):
                    nxt[m] = nxt[m] - first[i] * row_splat(sc, o + 80 + 8 * i + m)
        z = []
        for i in range(8):
            x = row_splat(sc, o + 64 + i)
            for p in range(i):
                x = x - low[i, p] * z[p]
            z.append(x * inv[i])
        z8 = z[7]
        for i in range(7):
            z8 = jnp.where(sub == i, z[i], z8)
        corner = jnp.zeros((8, SUB), F32)
        for m in range(8):
            x = d[m, m] * inv[m]
            for i in range(m):
                x = jnp.where(sub == i, low[m, i], x)
            corner = jnp.where(lane == j + m, x, corner)
        u_ref[j:j + 8, :] = jnp.where(lane >= j + 8, z8, jnp.where(lane >= sub + j, corner, 0.0))
        w_ref[j:j + 8, :] = jnp.where(lane < j + 8, z8, 0.0)
        for s in range(t + 1, end):
            c = first if s == t + 1 else column(s)
            x = jnp.where((lane >= j) & (lane < j + 8), 0.0, X[s])
            for i in range(8):
                x = x - c[i] * z[i]
            X[s] = x
        if t + 1 == half:
            e = 8 * half
            mid()
            top = u_ref[0:e, :]
            z = jnp.where(lax.broadcasted_iota(jnp.int32, (e, SUB), 1) < e, w_ref[0:e, :], top)
            prod = dot_hi(top[:, e:SUB], z, ((0,), (0,)))
            for s in range(half, n_oct):
                X[s] = jnp.where(lane < e, 0.0, X[s]) - prod[8 * (s - half):8 * (s - half + 1), :]
            nxt = [lane_splat(X[half], e + m) for m in range(8)]


def kernel(a_hbm, S, PQ, FB, D, ub, wb, sc, ld_sem, send_sem, p_sem, q_sem, fs_sem, fr_sem, us_sem, ur_sem):
    g = lax.axis_index("batch")
    r = lax.axis_index("row")
    c = lax.axis_index("col")
    n_q0 = 64
    same = r == lax.rem(c, 2)

    def blk(s):
        return pl.ds(pl.multiple_of(s * BS, SUB), BS)

    def p_idx(k, t):
        return 8 * k - (k // 2) * ((k + 1) // 2) + t - (k + 1) // 2

    def q_idx(k, s):
        m = k // 4
        return 4 * k - (4 * (m * (m - 1) // 2) + (k - 4 * m) * m) + s - m

    def first_t(k):
        return (k + 2 - r) // 2

    def to(row, col):
        return (g, row, col)

    def across(k):
        kc = lax.rem(k, 4)
        return jnp.where(lax.rem(kc, 2) == r, kc ^ 3, kc ^ 2)

    def p_copy(k, t, kind, col):
        i = p_idx(k, t)
        return pltpu.make_async_remote_copy(PQ.at[i], PQ.at[i], send_sem.at[kind, i], p_sem.at[i],
                                            device_id=to(r, col), device_id_type=MESH)

    def q_copy(k, t):
        i = p_idx(k, t)
        j = 2 * t + r
        q = q_idx(k, j // 4)
        return pltpu.make_async_remote_copy(PQ.at[i], PQ.at[n_q0 + q], send_sem.at[2, i], q_sem.at[q],
                                            device_id=to(1 - r, lax.rem(j, 4)), device_id_type=MESH)

    def p_local(k, t):
        i = p_idx(k, t)
        return pltpu.make_async_remote_copy(PQ.at[i], PQ.at[i], send_sem.at[0, i], p_sem.at[i],
                                            device_id=to(r, c ^ 1), device_id_type=MESH)

    def q_local(k, s):
        q = q_idx(k, s)
        return pltpu.make_async_remote_copy(PQ.at[n_q0 + q], PQ.at[n_q0 + q], send_sem.at[2, 0], q_sem.at[q],
                                            device_id=to(1 - r, c), device_id_type=MESH)

    def each_send(k, t, act):
        kc = lax.rem(k, 4)
        i = 2 * t + r
        j = lax.rem(i, 4)
        far = i > k + 1
        own = c == kc

        @pl.when(own & far)
        def _():
            act(p_copy(k, t, 1, across(k)))
            act(p_copy(k, t, 0, c ^ 1))

        @pl.when(own & (i < LAST) & (jnp.logical_not(far) | (j // 2 == kc // 2)))
        def _():
            act(q_copy(k, t))

        @pl.when((c == across(k)) & far)
        def _():
            act(p_copy(k, t, 0, c ^ 1))

            @pl.when((i < LAST) & (j == (c ^ 1)))
            def _():
                act(q_copy(k, t))

    def near_view(k, n):
        i = p_idx(k, (k + 1) // 2)
        if n < 2:
            return PQ.at[i, :, SUB * n:SUB * (n + 1)]
        return PQ.at[i, SUB * (n - 2):SUB * (n - 1), 2 * SUB:BS]

    def near_copy(k, n):
        return pltpu.make_async_remote_copy(near_view(k, n), near_view(k, n), us_sem.at[k, n], ur_sem.at[k, n],
                                            device_id=to(r, lax.rem(k + 1, 4)), device_id_type=MESH)

    def near_local(k, n):
        return pltpu.make_async_remote_copy(near_view(k, n), near_view(k, n), us_sem.at[k, n], ur_sem.at[k, n],
                                            device_id=to(r, lax.rem(k, 4)), device_id_type=MESH)

    def recv(k, t):
        p_local(k, t).wait_recv()

    def forward(k, t):
        recv(k, t)
        each_send(k, t, lambda cp: cp.start())

    def col_index(k, s):
        return jnp.where(same, p_idx(k, 2 * s + (c - r) // 2), n_q0 + q_idx(k, s))

    def update(k, t, s):
        @pl.when(k == 0)
        def _():
            load(t, s).wait()
        prod = lax.dot_general(PQ[p_idx(k, t)], PQ[col_index(k, s)], (((1,), (1,)), ((), ())),
                               preferred_element_type=F32)
        S[t, :, blk(s)] = S[t, :, blk(s)] - prod

    def fb_copy(slot, b):
        if b < 2:
            view = FB.at[slot, b, :, SUB * b:BS]
        else:
            view = FB.at[slot, 2, (b - 2) * SUB // 2:(b - 1) * SUB // 2, 2 * SUB:BS]
        return pltpu.make_async_remote_copy(view, view, fs_sem.at[slot, b], fr_sem.at[slot, b],
                                            device_id=to(1 - r, c), device_id_type=MESH)

    def load(t, s):
        return pltpu.make_async_copy(a_hbm.at[t, :, blk(s)], S.at[t, :, blk(s)], ld_sem.at[t, s])

    def lower(t, s):
        return 2 * t + r >= 4 * s + c

    def all_blocks(fn):
        def body(n, _):
            fn(lax.rem(n, 8), n // 8)
            return 0
        lax.fori_loop(0, 32, body, 0)

    def begin(t, s):
        @pl.when(lower(t, s))
        def _():
            load(t, s).start()

    def blank(t, s):
        @pl.when(jnp.logical_not(lower(t, s)))
        def _():
            S[t, :, blk(s)] = jnp.zeros((BS, BS), F32)

    barrier = pltpu.get_barrier_semaphore()
    all_blocks(begin)
    for step in range(1, 8):
        dr, dc = step // 4, step % 4
        pl.semaphore_signal(barrier, inc=1, device_id=to(r ^ dr, c ^ dc), device_id_type=MESH)
    pl.semaphore_wait(barrier, 7)

    def bf_dot(x, y):
        return lax.dot_general(x, y, (((1,), (1,)), ((), ())), preferred_element_type=F32)

    def shrink(row, col, part):
        D[row:row + SUB, col:BS] = D[row:row + SUB, col:BS] - bf_dot(part[row:row + SUB], part[col:BS])

    def factor_diag(slot, more, late):
        def tile(b, _):
            off = pl.multiple_of(b * SUB, SUB)
            def mid():
                @pl.when((b == 2) & more)
                def _():
                    FB[slot, 2, 0:SUB // 2, 2 * SUB:BS] = wb[0:SUB // 2, :]
                    fb_copy(slot, 2).start()

            factor_tile(D, off, ub.at[b], wb, sc, mid)
            w = wb[...]

            @pl.when(b < 2)
            def _():
                FB[slot, b, :, pl.ds(off, SUB)] = w

            @pl.when(b == 0)
            def _():
                late()
                rest = dot_hi(w, D[0:SUB, SUB:BS], ((1,), (0,)))
                FB[slot, 0, :, SUB:BS] = rest
                @pl.when(more)
                def _():
                    fb_copy(slot, 0).start()
                D[SUB:BS, SUB:BS] = D[SUB:BS, SUB:BS] - dot_hi(rest, rest, ((0,), (0,)))

            @pl.when(b == 1)
            def _():
                rest = dot_hi(w, D[SUB:2 * SUB, 2 * SUB:BS], ((1,), (0,)))
                FB[slot, 1, :, 2 * SUB:BS] = rest
                @pl.when(more)
                def _():
                    fb_copy(slot, 1).start()
                D[2 * SUB:BS, 2 * SUB:BS] = D[2 * SUB:BS, 2 * SUB:BS] - dot_hi(rest, rest, ((0,), (0,)))

            @pl.when(b == 2)
            def _():
                @pl.when(more)
                def _():
                    FB[slot, 2, SUB // 2:SUB, 2 * SUB:BS] = w[SUB // 2:SUB, :]
                    fb_copy(slot, 3).start()
            return 0
        lax.fori_loop(0, 3, tile, 0)

    def solve(k, t, s, ready, done, pieces):
        idx = p_idx(k, t)

        def tile(n):
            return pl.ds(pl.multiple_of(s * BS + SUB * n, SUB), SUB)

        def put(n, x):
            PQ[idx, :, SUB * n:SUB * (n + 1)] = x.astype(BF16)
            done(n)
            S[t, :, tile(n)] = x

        ready(0)
        x1 = dot_hi(S[t, :, tile(0)], FB[s, 0, :, 0:SUB], ((1,), (1,)))
        put(0, x1)
        rest = S[t, :, pl.ds(pl.multiple_of(s * BS + SUB, SUB), 2 * SUB)] - dot_hi(x1, FB[s, 0, :, SUB:BS], ((1,), (0,)))
        ready(1)
        x2 = dot_hi(rest[:, 0:SUB], FB[s, 1, :, SUB:2 * SUB], ((1,), (1,)))
        put(1, x2)
        last = rest[:, SUB:2 * SUB] - dot_hi(x2, FB[s, 1, :, 2 * SUB:BS], ((1,), (0,)))
        ready(2)
        rows = BS // pieces
        for h in range(pieces):
            at = slice(rows * h, rows * (h + 1))
            x3 = dot_hi(last[at], FB[s, 2, :, 2 * SUB:BS], ((1,), (1,)))
            PQ[idx, at, 2 * SUB:BS] = x3.astype(BF16)
            done(2 + h)
            S[t, at, tile(2)] = x3

    def wave(n, _):
        kd = n // MU
        sd = kd // 4
        td = kd // 2
        diag = (lax.rem(n, MU) == 0) & (c == lax.rem(kd, 4)) & (r == lax.rem(kd, 2))

        @pl.when(diag)
        def _():
            @pl.when(kd > 0)
            def _():
                @pl.when(kd == 1)
                def _():
                    load(td, sd).wait()
                D[...] = S[td, :, blk(sd)]
                idx = p_idx(kd - 1, td)
                for e in range(2):
                    near_local(kd - 1, e).wait_recv()
                    part = PQ[idx, :, SUB * e:SUB * (e + 1)]
                    for b in range(0, BS, SUB):
                        shrink(b, b, part)
                near_local(kd - 1, 2).wait_recv()
                top = PQ[idx, 0:SUB, 2 * SUB:BS]
                D[0:SUB, 0:SUB] = D[0:SUB, 0:SUB] - bf_dot(top, top)

            @pl.when(kd == 0)
            def _():
                load(td, sd).wait()
                D[...] = S[td, :, blk(sd)]

            def late():
                @pl.when(kd > 0)
                def _():
                    for e in range(3, 5):
                        near_local(kd - 1, e).wait_recv()
                    part = PQ[p_idx(kd - 1, td), :, 2 * SUB:BS]
                    shrink(0, SUB, part)
                    shrink(SUB, SUB, part)
                    shrink(2 * SUB, 2 * SUB, part)
            factor_diag(sd, kd < NB - 1, late)

        def span(v):
            par = lax.rem(v + r, 2)
            lo = (jnp.maximum(v - (NB - 1) + LAG - 1, 0) // LAG + 1 - par) // 2
            hi = ((v + MU - 2) // MU + 1 - par) // 2
            return par, lo, hi

        def pass_on(v):
            par, lo, hi = span(v)

            def one(m, _):
                k = 2 * m + par

                @pl.when(c == across(k))
                def _():
                    forward(k, (v - LAG * k - r) // 2)
                return 0
            lax.fori_loop(lo, hi, one, 0)

        @pl.when((n >= HOP) & ((lax.rem(n, MU) != 2) | (c != lax.rem(kd, 4)) | (r != lax.rem(kd + 1, 2))))
        def _():
            pass_on(n - HOP)

        near = (lax.rem(n, MU) == 1) & (c == lax.rem(kd, 4)) & (r == lax.rem(kd + 1, 2))

        @pl.when(near)
        def _():
            t = (kd + 1) // 2

            @pl.when(kd == 0)
            def _():
                load(t, sd).wait()

            @pl.when(kd > 0)
            def _():
                q_local(kd - 1, sd).wait_recv()

                @pl.when(lax.rem(kd, 2) == 1)
                def _():
                    recv(kd - 1, t)
                update(kd - 1, t, sd)

            def ready(e):
                if e == 1:
                    pass_on(n + 1 - HOP)
                fb_copy(sd, e).wait_recv()
                if e == 2:
                    fb_copy(sd, 3).wait_recv()
            solve(kd, t, sd, ready, lambda e: near_copy(kd, e).start(), 3)
            each_send(kd, t, lambda cp: cp.start())

        @pl.when(n >= LAG)
        def _():
            v = n - LAG
            par, lo, hi = span(v)
            hi = hi - jnp.where(near & (kd > 0), 1, 0)

            def arrive(m, _):
                k = 2 * m + par

                @pl.when((c != lax.rem(k, 4)) & (c != across(k)))
                def _():
                    recv(k, (v - LAG * k - r) // 2)
                return 0
            lax.fori_loop(lo, hi, arrive, 0)

            @pl.when(jnp.logical_not(same))
            def _():
                def arrive_q(s, _):
                    j = 4 * s + c
                    d = v - 1 - j

                    @pl.when((j < LAST) & (d >= 0) & (lax.rem(d, LAG) == 0) & (d < LAG * (j - 1)))
                    def _():
                        q_local(d // LAG, s).wait_recv()
                    return 0
                lax.fori_loop(0, 4, arrive_q, 0)

        @pl.when(lax.rem(n + c, 2) == r)
        def _():
            def task(m, _):
                s = 3 - m
                k = 4 * s + c
                i = n - LAG * k

                @pl.when((i > k + 1) & (i < NB))
                def _():
                    t = (i - r) // 2

                    @pl.when(k == 0)
                    def _():
                        load(t, s).wait()

                    @pl.when(k > 0)
                    def _():
                        update(k - 1, t, s)
                    solve(k, t, s, lambda e: None, lambda e: None, 1)
                    each_send(k, t, lambda cp: cp.start())
                return 0
            lax.fori_loop(0, 4, task, 0)

        @pl.when(n >= LAG)
        def _():
            v = n - LAG
            par, lo, hi = span(v)
            hi = hi - jnp.where(near & (kd > 0), 1, 0)

            def apply(m, _):
                k = 2 * m + par
                i = v - LAG * k

                def one(s, _):
                    @pl.when(4 * s + c != k + 1)
                    def _():
                        update(k, (i - r) // 2, s)
                    return 0
                lax.fori_loop((k + 4 - c) // 4, (i + 4 - c) // 4, one, 0)
                return 0
            lax.fori_loop(lo, hi, apply, 0)

        @pl.when(diag)
        def _():
            for b in range(3):
                S[td, SUB * b:SUB * (b + 1), pl.ds(pl.multiple_of(sd * BS + SUB * b, SUB), SUB)] = ub[b].T
                for e in range(b + 1, 3):
                    S[td, SUB * e:SUB * (e + 1), pl.ds(pl.multiple_of(sd * BS + SUB * b, SUB), SUB)] = FB[sd, b, :, SUB * e:SUB * (e + 1)].T
                    S[td, SUB * b:SUB * (b + 1), pl.ds(pl.multiple_of(sd * BS + SUB * e, SUB), SUB)] = jnp.zeros((SUB, SUB), F32)

        @pl.when(n == 2)
        def _():
            all_blocks(blank)
        return 0

    lax.fori_loop(0, MU * (NB - 1) + 1, wave, 0)

    def drain(k, _):
        t0 = first_t(k)
        own = c == lax.rem(k, 4)

        def one(t, _):
            each_send(k, t, lambda cp: cp.wait_send())
            return 0
        lax.fori_loop(t0, 8, one, 0)

        @pl.when(own & (k < NB - 1))
        def _():
            @pl.when(r == lax.rem(k, 2))
            def _():
                for b in range(4):
                    fb_copy(k // 4, b).wait_send()

            @pl.when(r != lax.rem(k, 2))
            def _():
                for b in range(5):
                    near_copy(k, b).wait_send()
        return 0
    lax.fori_loop(0, NB, drain, 0)


def solution(mesh):
    def local(a):
        return pl.pallas_call(
            kernel,
            out_shape=pltpu.VMEM(a.shape, F32),
            in_specs=[pl.BlockSpec(memory_space=pl.ANY)],
            out_specs=pl.BlockSpec(memory_space=pltpu.VMEM),
            scratch_shapes=[
                pltpu.VMEM((104, BS, BS), BF16),
                pltpu.VMEM((4, 3, SUB, BS), F32),
                pltpu.VMEM((BS, BS), F32),
                pltpu.VMEM((3, SUB, SUB), F32),
                pltpu.VMEM((SUB, SUB), F32),
                pltpu.VMEM((320, SUB), F32),
                pltpu.SemaphoreType.DMA((8, 4)),
                pltpu.SemaphoreType.DMA((3, 64)),
                pltpu.SemaphoreType.DMA((64,)),
                pltpu.SemaphoreType.DMA((40,)),
                pltpu.SemaphoreType.DMA((4, 4)),
                pltpu.SemaphoreType.DMA((4, 4)),
                pltpu.SemaphoreType.DMA((16, 5)),
                pltpu.SemaphoreType.DMA((16, 5)),
            ],
            compiler_params=pltpu.CompilerParams(collective_id=0, has_side_effects=True,
                                                 vmem_limit_bytes=44 * 2 ** 20),
            name="cholesky",
        )(a)

    spec = P(("batch", "row"), None, "col")
    return jax.shard_map(local, mesh=mesh, in_specs=(spec,), out_specs=spec, check_vma=False)
```
